32 devices in a mesh: row: 8 (over y, x, core), col: 4 (over z).
Axes of the slice: x: 2, y: 2, z: 4, core: 2. Of those that a mesh axis runs over, the one named last changes fastest.
Arguments:
- relief: float32 [3, 2048, 4096], P(None, 'row', 'col'), may hold values from -8 to 8
Outputs:
- level_one: float32 [3, 1024, 2048], P(None, 'row', 'col')
- level_two: float32 [3, 512, 1024], P(None, 'row', 'col')
- level_three: float32 [3, 256, 512], P(None, 'row', 'col')
- level_four: float32 [3, 128, 256], P(None, 'row', 'col')
The draws below stay inside these ranges and needn't reach their ends.
All inputs are finite; a program needn't handle non-finite values.
Results may differ from the reference program's by a relative error of at most 0.00002.
Values sent between devices are 32-bit elements; how exact they have to be, the bound alone decides.
No kernel may reach another device: no remote copies, remote signals or barrier semaphores. Data moves between devices by JAX's collectives and lax.ppermute only.
A program may use at most 64 MiB of HBM per device.

```python
import jax
import jax.numpy as jnp
from jax import lax

BANDS = 3
ROWS = 2048
COLS = 4096


def draw_relief(key, part):
    summed = jnp.zeros((BANDS, ROWS, COLS), jnp.float32)
    for octave in range(5):
        factor = 2 ** octave
        subkey = jax.random.fold_in(key, 11 + octave)
        coarse_noise = jnp.clip(jax.random.normal(subkey, (BANDS, ROWS // factor, COLS // factor), jnp.float32), -4.0, 4.0)
        summed = summed + jnp.repeat(jnp.repeat(coarse_noise, factor, 1), factor, 2)
    return jnp.clip(summed, -8.0, 8.0)


def setup_inputs(seed: int = 0) -> dict:
    key_list = jax.random.split(jax.random.key(seed), 2)
    relief = draw_relief(jax.random.fold_in(key_list[1], 71), 0)
    return dict(relief=relief)


binomial = (0.0625, 0.25, 0.375, 0.25, 0.0625)


def decimate(padded, along, extent):
    result = binomial[0] * lax.slice_in_dim(padded, 0, extent - 1, 2, along)
    for offset in range(1, 5):
        result = result + binomial[offset] * lax.slice_in_dim(padded, offset, offset + extent - 1, 2, along)
    return result


def reduce_along(field, along):
    extent = field.shape[along]
    widths = [(0, 0), (0, 0), (0, 0)]
    widths[along] = (2, 2)
    padded = jnp.pad(field, widths, mode="reflect")
    return decimate(padded, along, extent)


def reduce_level(field):
    return reduce_along(reduce_along(field, 1), 2)


def reference(relief):
    level_one = reduce_level(relief)
    level_two = reduce_level(level_one)
    level_three = reduce_level(level_two)
    level_four = reduce_level(level_three)
    return (level_one, level_two, level_three, level_four)
```

```python
import functools

import jax
import jax.numpy as jnp
from jax import lax
from jax.experimental import pallas as pl
from jax.experimental.pallas import tpu as pltpu
from jax.sharding import PartitionSpec as P

F32 = jnp.float32
BF16 = jnp.bfloat16
FAR = 1 << 20
LEVELS = 4
VMEM = pl.BlockSpec(memory_space=pltpu.VMEM)
PAD = 8
TAIL = 24


def lanes_of(cols):
    return (cols + 3 + 127) // 128 * 128


def iota(shape, dim):
    return lax.broadcasted_iota(jnp.int32, shape, dim)


def band(source, target):
    far = jnp.abs(source - 2 * target)
    return jnp.where(far == 0, 0.375, jnp.where(far == 1, 0.25, jnp.where(far == 2, 0.0625, 0.0))).astype(F32)


def block_matrix(first, last):
    source, lane = iota((256, 256), 0), iota((256, 256), 1)
    target = jnp.where(lane <= 128, lane, jnp.where(lane == 255, -1, FAR))
    value = band(source, target)
    if first is not None:
        value += first * jnp.where(source >= 1, band(-source, target), 0.0)
    if last is not None:
        value += last * jnp.where(source == 254, band(source + 2, target), 0.0)
    return value.astype(BF16)


def rim_matrix(first, last):
    source, lane = iota((128, 256), 0), iota((128, 256), 1)
    after = source < 64
    col = jnp.where(after, 512 + source, source - 128)
    own = jnp.where(lane < 2, 256 + lane, jnp.where(lane == 127, -1, FAR))
    other = jnp.where(lane == 128, 0, jnp.where(lane == 255, 255, FAR))
    value = band(col, jnp.where(lane < 128, own, other))
    keep = jnp.where(after, 1.0 - last, 1.0 - first)
    return (value * keep).astype(BF16)


def last_matrix(cols, first, last):
    source, lane = iota((2 * cols, cols), 0), iota((2 * cols, cols), 1)
    half = cols // 2
    col = jnp.where(source < cols + cols // 2, source, source - 2 * cols)
    target = jnp.where(lane < half + 2, lane, jnp.where(lane == cols - 1, -1, FAR))
    value = band(col, target)
    value += first * jnp.where((source >= 1) & (source < cols), band(-source, target), 0.0)
    value += last * jnp.where(source == cols - 2, band(source + 2, target), 0.0)
    keep = jnp.where(col < 0, 1.0 - first, jnp.where(col >= cols, 1.0 - last, 1.0))
    return (value * keep).astype(BF16)


def split_dot(value, matrix):
    high = value.astype(BF16)
    low = (value - high.astype(F32)).astype(BF16)
    return (
        jnp.dot(high, matrix, preferred_element_type=F32)
        + jnp.dot(low, matrix, preferred_element_type=F32)
    )


def columns(tiles, cols, matrices):
    blocks = cols // 256
    rim = len(tiles) > 2 * blocks
    parts = []
    for t in range(blocks):
        index = (1 if t == 0 else 0) + (2 if t == blocks - 1 else 0)
        value = jnp.concatenate(tiles[2 * t:2 * t + 2], 1)
        parts.append(split_dot(value, matrices[index][...]))
    near = iota((tiles[0].shape[0], 128), 1) < 64
    edges = [p[:, 128:] for p in parts]
    if rim:
        around = split_dot(tiles[-1], matrices[4][...])
        edges.append(around[:, 128:])
    else:
        edges.append(jnp.zeros_like(edges[0]))
    out = [
        parts[t][:, :128] + jnp.where(near, edges[t - 1], edges[t + 1])
        for t in range(blocks)
    ]
    outer = jnp.where(near, edges[blocks - 1], edges[0])
    if rim:
        outer = outer + around[:, :128]
    return out + [outer]


def rows(ref, extent):
    half = extent // 2

    def reduced(start, size):
        e = [ref[pl.ds(start + t, size, stride=2), :] for t in range(5)]
        return 0.0625 * (e[0] + e[4]) + 0.25 * (e[1] + e[3]) + 0.375 * e[2]

    main = reduced(PAD - 2, half)
    below = reduced(PAD - 2 + extent, 8)
    above = 0.25 * ref[PAD - 1:PAD, :] + 0.0625 * ref[PAD:PAD + 1, :]
    return jnp.concatenate([main, jnp.where(iota(below.shape, 0) == 7, above, below)], 0)


def close(ref, extent, first, last):
    @pl.when(first)
    def _():
        ref[:, PAD - 2:PAD - 1, :] = ref[:, PAD + 2:PAD + 3, :]
        ref[:, PAD - 1:PAD, :] = ref[:, PAD + 1:PAD + 2, :]

    @pl.when(last)
    def _():
        ref[:, PAD + extent:PAD + extent + 1, :] = ref[:, PAD + extent - 2:PAD + extent - 1, :]


def pyramid_kernel(
    shape, counts, x_hbm, one, two, three, four, rim_a, rim_b, send_e, send_o,
    s0, s1, s2, s3, mats, rim_mat, end_mat, sems,
):
    bands, n, m = shape
    row, col = lax.axis_index("row"), lax.axis_index("col")
    top, bottom = row == 0, row == counts[0] - 1
    copies = [
        [
            pltpu.make_async_copy(
                x_hbm.at[b, :, pl.ds(128 * t, 128)], s0.at[b, t, pl.ds(PAD, n), :], sems.at[b, t]
            )
            for t in range(m // 128)
        ]
        for b in range(bands)
    ]
    for copy in sum(copies, []):
        copy.start()
    left = jnp.where(col == 0, 1.0, 0.0).astype(F32)
    right = jnp.where(col == counts[1] - 1, 1.0, 0.0).astype(F32)
    mats[0] = block_matrix(None, None)
    mats[1] = block_matrix(left, None)
    mats[2] = block_matrix(None, right)
    mats[3] = block_matrix(left, right)
    rim_mat[...] = rim_matrix(left, right)
    end_mat[...] = last_matrix(end_mat.shape[1], left, right)
    matrices = [mats.at[i] for i in range(4)] + [rim_mat]
    fields, outs = [s0, s1, s2, s3], [one, two, three, four]
    for k, ref in enumerate(fields):
        extent = n >> k
        skip = 0 if k == 0 else 8
        if k == 0:
            ref[:, :, 0:PAD, :] = jnp.zeros(ref.shape[:2] + (PAD, 128), F32)
        ref[:, :, PAD + extent + skip:, :] = jnp.zeros(ref.shape[:2] + (TAIL - skip, 128), F32)
    rim_b[...] = jnp.zeros_like(rim_b)
    down = [[jnp.zeros((8, 128), F32)] * (lanes_of(m >> (k + 1)) // 128) for k in range(LEVELS)]
    up = [list(d) for d in down]
    sub = iota((8, 128), 0)
    for k in range(LEVELS):
        extent, cols = n >> k, m >> k
        half = extent // 2
        for b in range(bands):
            if k == 0:
                for copy in copies[b]:
                    copy.wait()
            close(fields[k].at[b], extent, top, bottom)
            tiles = [rows(fields[k].at[b, t], extent) for t in range(fields[k].shape[1])]
            if k < LEVELS - 1:
                tiles = columns(tiles, cols, matrices)
            else:
                tiles = [split_dot(jnp.concatenate(tiles, 1), end_mat[...])]
            for t, tile in enumerate(tiles):
                body, tail = tile[:half], tile[half:]
                if k < LEVELS - 1:
                    after = fields[k + 1]
                    after[b, t, PAD:PAD + half, :] = body
                    after[b, t, 0:PAD, :] = jnp.where(sub == 7, tail, 0.0)
                    after[b, t, PAD + half:PAD + half + 8, :] = jnp.where(sub < 2, tail, 0.0)
                    if t < len(tiles) - 1:
                        outs[k][b, :, 128 * t:128 * t + 128] = body
                moved = pltpu.roll(tail, 2 * b, 0) if b else tail
                down[k][t] = jnp.where((sub >= 2 * b) & (sub < 2 * b + 2), moved, down[k][t])
                up[k][t] = jnp.where(sub == 2 * b, pltpu.roll(tail, 2 * b + 1, 0), up[k][t])
            body = tiles[-1][:half]
            start = sum(n >> j for j in range(2, k + 1))
            if k == LEVELS - 1:
                four[b] = body[:, :cols // 2]
                body = jnp.where(iota(body.shape, 1) < 2, pltpu.roll(body, 128 - cols // 2, 1), body)
            if k == 0:
                rim_a[b] = body
            else:
                rim_b[b, start:start + half, :] = body
    down, up = jnp.concatenate(sum(down, []), 1), jnp.concatenate(sum(up, []), 1)
    even = (row & 1) == 0
    send_e[...] = jnp.where(even, down, up)
    send_o[...] = jnp.where(even, up, down)


def from_rows(got_e, got_o):
    even = (lax.axis_index("row") & 1) == 0
    e, o = got_e[...], got_o[...]
    return jnp.where(even, o, e), jnp.where(even, e, o)


def upper(part, b):
    part = pltpu.roll(part, 8 - 2 * b, 0) if b else part
    return jnp.where(iota(part.shape, 0) < 2, part, 0.0)


def lower(part, b):
    part = pltpu.roll(part, 7 - 2 * b, 0)
    return jnp.where(iota(part.shape, 0) == 7, part, 0.0)


def segments(n):
    out, start = [], 0
    for k in range(2, LEVELS + 1):
        out.append((k, start, n >> k))
        start += n >> k
    return out


def rim_kernel(shape, rim_a, rim_b, got_e, got_o, send_e, send_o, tile_a, tile_b):
    bands, n, m = shape
    above, below = from_rows(got_e, got_o)
    offsets, start = [], 0
    for k in range(1, LEVELS + 1):
        cols = m >> k
        offsets.append(start + (cols if cols >= 128 else 0))
        start += lanes_of(cols)

    def rim_of(part, k):
        part = part[:, offsets[k - 1]:offsets[k - 1] + 128]
        if (m >> k) < 128:
            part = jnp.where(iota(part.shape, 1) < 2, pltpu.roll(part, 128 - (m >> k), 1), part)
        return part

    sub = iota((16, 128), 0)
    to_right, to_left = jnp.zeros((16, 128), F32), jnp.zeros((16, 128), F32)
    for b in range(bands):
        half = n // 2
        tile_a[b] = rim_a[b]
        tile_b[b] = rim_b[b]
        for ref, k, first, size in [(tile_a, 1, 0, half)] + [(tile_b, k, s, z) for k, s, z in segments(n)]:
            ref[b, first:first + 8, :] += upper(rim_of(above, k), b)
            ref[b, first + size - 8:first + size, :] += lower(rim_of(below, k), b)
        a = jnp.transpose(tile_a[b])
        c = jnp.transpose(tile_b[b])
        to_right = jnp.where(sub == 4 * b, a[0:1], to_right)
        to_right = jnp.where(sub == 4 * b + 1, c[0:1], to_right)
        to_right = jnp.where(sub == 4 * b + 2, c[1:2], to_right)
        to_left = jnp.where(sub == 4 * b, a[127:128], to_left)
        to_left = jnp.where(sub == 4 * b + 1, c[127:128], to_left)
    even = (lax.axis_index("col") & 1) == 0
    send_e[...] = jnp.where(even, to_right, to_left)
    send_o[...] = jnp.where(even, to_left, to_right)


def finish_kernel(
    shape, one, two, three, four, row_e, row_o, col_e, col_o,
    out_one, out_two, out_three, out_four, tile_a, tile_b,
):
    bands, n, m = shape
    above, below = from_rows(row_e, row_o)
    even = (lax.axis_index("col") & 1) == 0
    before = jnp.where(even, col_o[...], col_e[...])
    after = jnp.where(even, col_e[...], col_o[...])
    fields, outs = [one, two, three, four], [out_one, out_two, out_three, out_four]
    tile_a[...] = jnp.zeros_like(tile_a)
    tile_b[...] = jnp.zeros_like(tile_b)
    lane = iota((128, 128), 1)
    for b in range(bands):
        tile_a[b, 0:1, :] = before[4 * b:4 * b + 1]
        tile_a[b, 127:128, :] = after[4 * b:4 * b + 1]
        tile_b[b, 0:2, :] = before[4 * b + 1:4 * b + 3]
        tile_b[b, 127:128, :] = after[4 * b + 1:4 * b + 2]
        tile_b[b, 63:64, :] = after[4 * b + 1:4 * b + 2]
        a = jnp.transpose(tile_a[b])
        c = jnp.transpose(tile_b[b])
        start = 0
        for k, first, size in [(1, 0, n // 2)] + segments(n):
            cols = m >> k
            part = (a if k == 1 else c)[first:first + size]
            wide = min(cols, 128)
            spot = lane[:size, :wide]
            part = part[:, :wide]
            low, high = jnp.where(spot < 2, part, 0.0), jnp.where(spot == wide - 1, part, 0.0)
            for t in range(cols // wide):
                at = pl.ds(wide * t, wide)
                value = fields[k - 1][b, :, at]
                if t == 0:
                    value = value + low
                if t == cols // wide - 1:
                    value = value + high
                outs[k - 1][b, :, at] = value
            top = upper(above[:, start:start + cols], b)
            end = lower(below[:, start:start + cols], b)
            outs[k - 1][b, 0:8, :] += top
            outs[k - 1][b, size - 8:size, :] += end
            start += lanes_of(cols)


def swap(value, axis):
    e, o = value
    count = lax.axis_size(axis)
    pairs = [[], []]
    for i in range(count - 1):
        pairs[i % 2] += [(i, i + 1), (i + 1, i)]
    return lax.ppermute(e, axis, pairs[0]), lax.ppermute(o, axis, pairs[1])


def solution(mesh):
    counts = (mesh.shape["row"], mesh.shape["col"])

    def local(relief):
        shape = bands, n, m = relief.shape
        levels = [jax.ShapeDtypeStruct((bands, n >> k, m >> k), F32) for k in range(1, LEVELS + 1)]
        width = sum(lanes_of(m >> k) for k in range(1, LEVELS + 1))
        row_part = jax.ShapeDtypeStruct((8, width), F32)
        col_part = jax.ShapeDtypeStruct((16, 128), F32)
        rim = jax.ShapeDtypeStruct((bands, 128, 128), F32)
        *own, rim_a, rim_b, send_e, send_o = pl.pallas_call(
            functools.partial(pyramid_kernel, shape, counts),
            out_shape=levels + [rim, rim, row_part, row_part],
            in_specs=[pl.BlockSpec(memory_space=pl.ANY)],
            out_specs=[VMEM] * 8,
            scratch_shapes=[
                pltpu.VMEM((bands, (lanes_of(m >> k) if k else m) // 128, PAD + (n >> k) + TAIL, 128), F32)
                for k in range(LEVELS)
            ] + [
                pltpu.VMEM((4, 256, 256), BF16),
                pltpu.VMEM((128, 256), BF16),
                pltpu.VMEM((m >> 2, m >> 3), BF16),
                pltpu.SemaphoreType.DMA((bands, m // 128)),
            ],
            name="pyramid",
        )(relief)
        row_e, row_o = swap((send_e, send_o), "row")
        send_e, send_o = pl.pallas_call(
            functools.partial(rim_kernel, shape),
            out_shape=[col_part, col_part],
            in_specs=[VMEM] * 4,
            out_specs=[VMEM] * 2,
            scratch_shapes=[pltpu.VMEM((bands, 128, 128), F32)] * 2,
            name="rim",
        )(rim_a, rim_b, row_e, row_o)
        col_e, col_o = swap((send_e, send_o), "col")
        return tuple(pl.pallas_call(
            functools.partial(finish_kernel, shape),
            out_shape=levels,
            in_specs=[VMEM] * 8,
            out_specs=[VMEM] * 4,
            scratch_shapes=[pltpu.VMEM((bands, 128, 128), F32)] * 2,
            name="finish",
        )(*own, row_e, row_o, col_e, col_o))

    placed = P(None, "row", "col")
    return jax.shard_map(
        local, mesh=mesh, in_specs=(placed,), out_specs=(placed,) * LEVELS, check_vma=False
    )
```

```python
import functools

import jax
import jax.numpy as jnp
from jax import lax
from jax.experimental import pallas as pl
from jax.experimental.pallas import tpu as pltpu
from jax.sharding import PartitionSpec as P

F32 = jnp.float32
BF16 = jnp.bfloat16
FAR = 1 << 20
LEVELS = 4
LIMIT = 24_000_000
VMEM = pl.BlockSpec(memory_space=pltpu.VMEM)
PAD = 8
TAIL = 24


def lanes_of(cols):
    return (cols + 3 + 127) // 128 * 128


def iota(shape, dim):
    return lax.broadcasted_iota(jnp.int32, shape, dim)


def band(source, target):
    far = jnp.abs(source - 2 * target)
    return jnp.where(far == 0, 0.375, jnp.where(far == 1, 0.25, jnp.where(far == 2, 0.0625, 0.0))).astype(F32)


def block_matrix(first, last):
    source, lane = iota((256, 256), 0), iota((256, 256), 1)
    target = jnp.where(lane <= 128, lane, jnp.where(lane == 255, -1, FAR))
    value = band(source, target)
    if first is not None:
        value += first * jnp.where(source >= 1, band(-source, target), 0.0)
    if last is not None:
        value += last * jnp.where(source == 254, band(source + 2, target), 0.0)
    return value.astype(BF16)


def rim_matrix(first, last):
    source, lane = iota((128, 256), 0), iota((128, 256), 1)
    after = source < 64
    col = jnp.where(after, 512 + source, source - 128)
    own = jnp.where(lane < 2, 256 + lane, jnp.where(lane == 127, -1, FAR))
    other = jnp.where(lane == 128, 0, jnp.where(lane == 255, 255, FAR))
    value = band(col, jnp.where(lane < 128, own, other))
    keep = jnp.where(after, 1.0 - last, 1.0 - first)
    return (value * keep).astype(BF16)


def last_matrix(cols, first, last):
    source, lane = iota((2 * cols, cols), 0), iota((2 * cols, cols), 1)
    half = cols // 2
    col = jnp.where(source < cols + cols // 2, source, source - 2 * cols)
    target = jnp.where(lane < half + 2, lane, jnp.where(lane == cols - 1, -1, FAR))
    value = band(col, target)
    value += first * jnp.where((source >= 1) & (source < cols), band(-source, target), 0.0)
    value += last * jnp.where(source == cols - 2, band(source + 2, target), 0.0)
    keep = jnp.where(col < 0, 1.0 - first, jnp.where(col >= cols, 1.0 - last, 1.0))
    return (value * keep).astype(BF16)


def split_dot(value, matrix):
    high = value.astype(BF16)
    low = (value - high.astype(F32)).astype(BF16)
    return (
        jnp.dot(high, matrix, preferred_element_type=F32)
        + jnp.dot(low, matrix, preferred_element_type=F32)
    )


def columns(tiles, cols, matrices):
    blocks = cols // 256
    rim = len(tiles) > 2 * blocks
    parts = []
    for t in range(blocks):
        index = (1 if t == 0 else 0) + (2 if t == blocks - 1 else 0)
        value = jnp.concatenate(tiles[2 * t:2 * t + 2], 1)
        parts.append(split_dot(value, matrices[index][...]))
    near = iota((tiles[0].shape[0], 128), 1) < 64
    edges = [p[:, 128:] for p in parts]
    if rim:
        around = split_dot(tiles[-1], matrices[4][...])
        edges.append(around[:, 128:])
    else:
        edges.append(jnp.zeros_like(edges[0]))
    out = [
        parts[t][:, :128] + jnp.where(near, edges[t - 1], edges[t + 1])
        for t in range(blocks)
    ]
    outer = jnp.where(near, edges[blocks - 1], edges[0])
    if rim:
        outer = outer + around[:, :128]
    return out + [outer]


def rows(ref, extent):
    half = extent // 2

    def reduced(start, size):
        e = [ref[pl.ds(start + t, size, stride=2), :] for t in range(5)]
        return 0.0625 * (e[0] + e[4]) + 0.25 * (e[1] + e[3]) + 0.375 * e[2]

    main = reduced(PAD - 2, half)
    below = reduced(PAD - 2 + extent, 8)
    above = 0.25 * ref[PAD - 1:PAD, :] + 0.0625 * ref[PAD:PAD + 1, :]
    return jnp.concatenate([main, jnp.where(iota(below.shape, 0) == 7, above, below)], 0)


def close(ref, extent, first, last):
    @pl.when(first)
    def _():
        ref[:, PAD - 2:PAD - 1, :] = ref[:, PAD + 2:PAD + 3, :]
        ref[:, PAD - 1:PAD, :] = ref[:, PAD + 1:PAD + 2, :]

    @pl.when(last)
    def _():
        ref[:, PAD + extent:PAD + extent + 1, :] = ref[:, PAD + extent - 2:PAD + extent - 1, :]


def pyramid_kernel(
    shape, counts, x_hbm, one, two, three, four, rim_a, rim_b, send_e, send_o,
    s0, s1, s2, s3, mats, rim_mat, end_mat, sems,
):
    bands, n, m = shape
    row, col = lax.axis_index("row"), lax.axis_index("col")
    top, bottom = row == 0, row == counts[0] - 1
    copies = [
        [
            pltpu.make_async_copy(
                x_hbm.at[b, :, pl.ds(128 * t, 128)], s0.at[b, t, pl.ds(PAD, n), :], sems.at[b, t]
            )
            for t in range(m // 128)
        ]
        for b in range(bands)
    ]
    for copy in sum(copies, []):
        copy.start()
    left = jnp.where(col == 0, 1.0, 0.0).astype(F32)
    right = jnp.where(col == counts[1] - 1, 1.0, 0.0).astype(F32)
    mats[0] = block_matrix(None, None)
    mats[1] = block_matrix(left, None)
    mats[2] = block_matrix(None, right)
    mats[3] = block_matrix(left, right)
    rim_mat[...] = rim_matrix(left, right)
    end_mat[...] = last_matrix(end_mat.shape[1], left, right)
    matrices = [mats.at[i] for i in range(4)] + [rim_mat]
    fields, outs = [s0, s1, s2, s3], [one, two, three, four]
    for k, ref in enumerate(fields):
        extent = n >> k
        skip = 0 if k == 0 else 8
        if k == 0:
            ref[:, :, 0:PAD, :] = jnp.zeros(ref.shape[:2] + (PAD, 128), F32)
        ref[:, :, PAD + extent + skip:, :] = jnp.zeros(ref.shape[:2] + (TAIL - skip, 128), F32)
    rim_b[...] = jnp.zeros_like(rim_b)
    down = [[jnp.zeros((8, 128), F32)] * (lanes_of(m >> (k + 1)) // 128) for k in range(LEVELS)]
    up = [list(d) for d in down]
    sub = iota((8, 128), 0)
    for k in range(LEVELS):
        extent, cols = n >> k, m >> k
        half = extent // 2
        for b in range(bands):
            if k == 0:
                for copy in copies[b]:
                    copy.wait()
            close(fields[k].at[b], extent, top, bottom)
            tiles = [rows(fields[k].at[b, t], extent) for t in range(fields[k].shape[1])]
            if k < LEVELS - 1:
                tiles = columns(tiles, cols, matrices)
            else:
                tiles = [split_dot(jnp.concatenate(tiles, 1), end_mat[...])]
            for t, tile in enumerate(tiles):
                body, tail = tile[:half], tile[half:]
                if k < LEVELS - 1:
                    after = fields[k + 1]
                    after[b, t, PAD:PAD + half, :] = body
                    after[b, t, 0:PAD, :] = jnp.where(sub == 7, tail, 0.0)
                    after[b, t, PAD + half:PAD + half + 8, :] = jnp.where(sub < 2, tail, 0.0)
                    if t < len(tiles) - 1:
                        outs[k][b, :, 128 * t:128 * t + 128] = body
                moved = pltpu.roll(tail, 2 * b, 0) if b else tail
                down[k][t] = jnp.where((sub >= 2 * b) & (sub < 2 * b + 2), moved, down[k][t])
                up[k][t] = jnp.where(sub == 2 * b, pltpu.roll(tail, 2 * b + 1, 0), up[k][t])
            body = tiles[-1][:half]
            start = sum(n >> j for j in range(2, k + 1))
            if k == LEVELS - 1:
                four[b] = body[:, :cols // 2]
                body = jnp.where(iota(body.shape, 1) < 2, pltpu.roll(body, 128 - cols // 2, 1), body)
            if k == 0:
                rim_a[b] = body
            else:
                rim_b[b, start:start + half, :] = body
    down, up = jnp.concatenate(sum(down, []), 1), jnp.concatenate(sum(up, []), 1)
    down, up = jnp.where(bottom, 0.0, down), jnp.where(top, 0.0, up)
    even = (row & 1) == 0
    send_e[...] = jnp.where(even, down, up)
    send_o[...] = jnp.where(even, up, down)


def from_rows(got_e, got_o):
    even = (lax.axis_index("row") & 1) == 0
    e, o = got_e[...], got_o[...]
    return jnp.where(even, o, e), jnp.where(even, e, o)


def upper(part, b):
    part = pltpu.roll(part, 8 - 2 * b, 0) if b else part
    return jnp.where(iota(part.shape, 0) < 2, part, 0.0)


def lower(part, b):
    part = pltpu.roll(part, 7 - 2 * b, 0)
    return jnp.where(iota(part.shape, 0) == 7, part, 0.0)


def segments(n):
    out, start = [], 0
    for k in range(2, LEVELS + 1):
        out.append((k, start, n >> k))
        start += n >> k
    return out


def rim_kernel(shape, counts, rim_a, rim_b, got_e, got_o, send_e, send_o, tile_a, tile_b):
    bands, n, m = shape
    above, below = from_rows(got_e, got_o)
    offsets, start = [], 0
    for k in range(1, LEVELS + 1):
        cols = m >> k
        offsets.append(start + (cols if cols >= 128 else 0))
        start += lanes_of(cols)

    def rim_of(part, k):
        part = part[:, offsets[k - 1]:offsets[k - 1] + 128]
        if (m >> k) < 128:
            part = jnp.where(iota(part.shape, 1) < 2, pltpu.roll(part, 128 - (m >> k), 1), part)
        return part

    sub = iota((16, 128), 0)
    to_right, to_left = jnp.zeros((16, 128), F32), jnp.zeros((16, 128), F32)
    for b in range(bands):
        half = n // 2
        tile_a[b] = rim_a[b]
        tile_b[b] = rim_b[b]
        for ref, k, first, size in [(tile_a, 1, 0, half)] + [(tile_b, k, s, z) for k, s, z in segments(n)]:
            ref[b, first:first + 8, :] += upper(rim_of(above, k), b)
            ref[b, first + size - 8:first + size, :] += lower(rim_of(below, k), b)
        a = jnp.transpose(tile_a[b])
        c = jnp.transpose(tile_b[b])
        to_right = jnp.where(sub == 4 * b, a[0:1], to_right)
        to_right = jnp.where(sub == 4 * b + 1, c[0:1], to_right)
        to_right = jnp.where(sub == 4 * b + 2, c[1:2], to_right)
        to_left = jnp.where(sub == 4 * b, a[127:128], to_left)
        to_left = jnp.where(sub == 4 * b + 1, c[127:128], to_left)
    col = lax.axis_index("col")
    to_right = jnp.where(col == counts[1] - 1, 0.0, to_right)
    to_left = jnp.where(col == 0, 0.0, to_left)
    even = (col & 1) == 0
    send_e[...] = jnp.where(even, to_right, to_left)
    send_o[...] = jnp.where(even, to_left, to_right)


def finish_kernel(
    shape, one, two, three, four, row_e, row_o, col_e, col_o,
    out_one, out_two, out_three, out_four, tile_a, tile_b,
):
    bands, n, m = shape
    above, below = from_rows(row_e, row_o)
    even = (lax.axis_index("col") & 1) == 0
    before = jnp.where(even, col_o[...], col_e[...])
    after = jnp.where(even, col_e[...], col_o[...])
    fields, outs = [one, two, three, four], [out_one, out_two, out_three, out_four]
    tile_a[...] = jnp.zeros_like(tile_a)
    tile_b[...] = jnp.zeros_like(tile_b)
    lane = iota((128, 128), 1)
    for b in range(bands):
        tile_a[b, 0:1, :] = before[4 * b:4 * b + 1]
        tile_a[b, 127:128, :] = after[4 * b:4 * b + 1]
        tile_b[b, 0:2, :] = before[4 * b + 1:4 * b + 3]
        tile_b[b, 127:128, :] = after[4 * b + 1:4 * b + 2]
        tile_b[b, 63:64, :] = after[4 * b + 1:4 * b + 2]
        a = jnp.transpose(tile_a[b])
        c = jnp.transpose(tile_b[b])
        start = 0
        for k, first, size in [(1, 0, n // 2)] + segments(n):
            cols = m >> k
            part = (a if k == 1 else c)[first:first + size]
            wide = min(cols, 128)
            spot = lane[:size, :wide]
            part = part[:, :wide]
            low, high = jnp.where(spot < 2, part, 0.0), jnp.where(spot == wide - 1, part, 0.0)
            for t in range(cols // wide):
                at = pl.ds(wide * t, wide)
                value = fields[k - 1][b, :, at]
                if t == 0:
                    value = value + low
                if t == cols // wide - 1:
                    value = value + high
                outs[k - 1][b, :, at] = value
            top = upper(above[:, start:start + cols], b)
            end = lower(below[:, start:start + cols], b)
            outs[k - 1][b, 0:8, :] += top
            outs[k - 1][b, size - 8:size, :] += end
            start += lanes_of(cols)


def swap(pair, axis, counts):
    sizes = [counts[name] for name in ("row", "col")]
    along = ("row", "col").index(axis)
    out = []
    for parity, value in enumerate(pair):
        moves = []
        for i in range(sizes[0] * sizes[1]):
            place = list(divmod(i, sizes[1]))
            step = 1 if place[along] % 2 == parity else -1
            target = list(place)
            if 0 <= place[along] + step < sizes[along]:
                target[along] += step
            elif (place[1 - along] ^ 1) < sizes[1 - along]:
                target[1 - along] ^= 1
            else:
                continue
            moves.append((i, target[0] * sizes[1] + target[1]))
        out.append(lax.ppermute(value, ("row", "col"), moves))
    return out


def solution(mesh):
    counts = (mesh.shape["row"], mesh.shape["col"])

    def local(relief):
        shape = bands, n, m = relief.shape
        levels = [jax.ShapeDtypeStruct((bands, n >> k, m >> k), F32) for k in range(1, LEVELS + 1)]
        width = sum(lanes_of(m >> k) for k in range(1, LEVELS + 1))
        row_part = jax.ShapeDtypeStruct((8, width), F32)
        col_part = jax.ShapeDtypeStruct((16, 128), F32)
        rim = jax.ShapeDtypeStruct((bands, 128, 128), F32)
        *own, rim_a, rim_b, send_e, send_o = pl.pallas_call(
            functools.partial(pyramid_kernel, shape, counts),
            out_shape=levels + [rim, rim, row_part, row_part],
            in_specs=[pl.BlockSpec(memory_space=pltpu.HBM)],
            out_specs=[VMEM] * 8,
            scratch_shapes=[
                pltpu.VMEM((bands, (lanes_of(m >> k) if k else m) // 128, PAD + (n >> k) + TAIL, 128), F32)
                for k in range(LEVELS)
            ] + [
                pltpu.VMEM((4, 256, 256), BF16),
                pltpu.VMEM((128, 256), BF16),
                pltpu.VMEM((m >> 2, m >> 3), BF16),
                pltpu.SemaphoreType.DMA((bands, m // 128)),
            ],
            compiler_params=pltpu.CompilerParams(vmem_limit_bytes=LIMIT),
            name="pyramid",
        )(pltpu.with_memory_space_constraint(relief, pltpu.HBM))
        row_e, row_o = swap((send_e, send_o), "row", mesh.shape)
        send_e, send_o = pl.pallas_call(
            functools.partial(rim_kernel, shape, counts),
            out_shape=[col_part, col_part],
            in_specs=[VMEM] * 4,
            out_specs=[VMEM] * 2,
            scratch_shapes=[pltpu.VMEM((bands, 128, 128), F32)] * 2,
            compiler_params=pltpu.CompilerParams(vmem_limit_bytes=4 << 20),
            name="rim",
        )(rim_a, rim_b, row_e, row_o)
        col_e, col_o = swap((send_e, send_o), "col", mesh.shape)
        return tuple(pl.pallas_call(
            functools.partial(finish_kernel, shape),
            out_shape=levels,
            in_specs=[VMEM] * 8,
            out_specs=[VMEM] * 4,
            scratch_shapes=[pltpu.VMEM((bands, 128, 128), F32)] * 2,
            compiler_params=pltpu.CompilerParams(vmem_limit_bytes=8 << 20),
            name="finish",
        )(*own, row_e, row_o, col_e, col_o))

    placed = P(None, "row", "col")
    return jax.shard_map(
        local, mesh=mesh, in_specs=(placed,), out_specs=(placed,) * LEVELS, check_vma=False
    )
```

```python
import functools

import jax
import jax.numpy as jnp
from jax import lax
from jax.experimental import pallas as pl
from jax.experimental.pallas import tpu as pltpu
from jax.sharding import PartitionSpec as P

F32 = jnp.float32
BF16 = jnp.bfloat16
FAR = 1 << 20
LEVELS = 4
LIMIT = 24_000_000
VMEM = pl.BlockSpec(memory_space=pltpu.VMEM)
PAD = 8
TAIL = 24


def lanes_of(cols):
    return (cols + 3 + 127) // 128 * 128


def iota(shape, dim):
    return lax.broadcasted_iota(jnp.int32, shape, dim)


def band(source, target):
    far = jnp.abs(source - 2 * target)
    return jnp.where(far == 0, 0.375, jnp.where(far == 1, 0.25, jnp.where(far == 2, 0.0625, 0.0))).astype(F32)


def fill_blocks(mats, first, last):
    source, lane = iota((256, 256), 0), iota((256, 256), 1)
    target = jnp.where(lane <= 128, lane, jnp.where(lane == 255, -1, FAR))
    value = band(source, target)
    inside = value.astype(BF16)
    for i in range(4):
        mats[i] = inside
    source, target = iota((16, 128), 0), iota((16, 128), 1)
    mirror = jnp.where(source >= 1, band(-source, target), 0.0)
    start = (value[:16, :128] + first * mirror).astype(BF16)
    source = source + 240
    mirror = jnp.where(source == 254, band(source + 2, target), 0.0)
    end = (value[240:, :128] + last * mirror).astype(BF16)
    for i in (1, 3):
        mats[i, :16, :128] = start
    for i in (2, 3):
        mats[i, 240:, :128] = end


def rim_matrix(first, last):
    source, lane = iota((128, 256), 0), iota((128, 256), 1)
    after = source < 64
    col = jnp.where(after, 512 + source, source - 128)
    own = jnp.where(lane < 2, 256 + lane, jnp.where(lane == 127, -1, FAR))
    other = jnp.where(lane == 128, 0, jnp.where(lane == 255, 255, FAR))
    value = band(col, jnp.where(lane < 128, own, other))
    keep = jnp.where(after, 1.0 - last, 1.0 - first)
    return (value * keep).astype(BF16)


def last_matrix(cols, first, last):
    source, lane = iota((2 * cols, cols), 0), iota((2 * cols, cols), 1)
    half = cols // 2
    col = jnp.where(source < cols + cols // 2, source, source - 2 * cols)
    target = jnp.where(lane < half + 2, lane, jnp.where(lane == cols - 1, -1, FAR))
    value = band(col, target)
    value += first * jnp.where((source >= 1) & (source < cols), band(-source, target), 0.0)
    value += last * jnp.where(source == cols - 2, band(source + 2, target), 0.0)
    keep = jnp.where(col < 0, 1.0 - first, jnp.where(col >= cols, 1.0 - last, 1.0))
    return (value * keep).astype(BF16)


def split_dot(value, matrix):
    high = value.astype(BF16)
    low = (value - high.astype(F32)).astype(BF16)
    return (
        jnp.dot(high, matrix, preferred_element_type=F32)
        + jnp.dot(low, matrix, preferred_element_type=F32)
    )


def columns(tiles, cols, matrices):
    blocks = cols // 256
    rim = len(tiles) > 2 * blocks
    parts = []
    for t in range(blocks):
        index = (1 if t == 0 else 0) + (2 if t == blocks - 1 else 0)
        value = jnp.concatenate(tiles[2 * t:2 * t + 2], 1)
        parts.append(split_dot(value, matrices[index][...]))
    near = iota((tiles[0].shape[0], 128), 1) < 64
    edges = [p[:, 128:] for p in parts]
    if rim:
        around = split_dot(tiles[-1], matrices[4][...])
        edges.append(around[:, 128:])
    else:
        edges.append(jnp.zeros_like(edges[0]))
    out = [
        parts[t][:, :128] + jnp.where(near, edges[t - 1], edges[t + 1])
        for t in range(blocks)
    ]
    outer = jnp.where(near, edges[blocks - 1], edges[0])
    if rim:
        outer = outer + around[:, :128]
    return out + [outer]


def rows(ref, extent):
    half = extent // 2

    def reduced(start, size):
        e = [ref[pl.ds(start + t, size, stride=2), :] for t in range(5)]
        return 0.0625 * (e[0] + e[4]) + 0.25 * (e[1] + e[3]) + 0.375 * e[2]

    main = reduced(PAD - 2, half)
    below = reduced(PAD - 2 + extent, 8)
    above = 0.25 * ref[PAD - 1:PAD, :] + 0.0625 * ref[PAD:PAD + 1, :]
    return jnp.concatenate([main, jnp.where(iota(below.shape, 0) == 7, above, below)], 0)


def close(ref, extent, first, last):
    @pl.when(first)
    def _():
        ref[:, PAD - 2:PAD - 1, :] = ref[:, PAD + 2:PAD + 3, :]
        ref[:, PAD - 1:PAD, :] = ref[:, PAD + 1:PAD + 2, :]

    @pl.when(last)
    def _():
        ref[:, PAD + extent:PAD + extent + 1, :] = ref[:, PAD + extent - 2:PAD + extent - 1, :]


HEAD, FOOT = 16, 32


def edge_kernel(
    shape, counts, x_hbm, send_e, send_o, s0, mats, rim_mat, end_mat,
    raw, e0, e1, e2, e3, down, up, edge_sems, sems,
):
    bands, n, m = shape
    row, col = lax.axis_index("row"), lax.axis_index("col")
    top, bottom = row == 0, row == counts[0] - 1
    near = [
        pltpu.make_async_copy(x_hbm.at[:, pl.ds(0, HEAD), :], raw.at[:, pl.ds(0, HEAD), :], edge_sems.at[0]),
        pltpu.make_async_copy(x_hbm.at[:, pl.ds(n - FOOT, FOOT), :], raw.at[:, pl.ds(HEAD, FOOT), :], edge_sems.at[1]),
    ]
    whole = [
        pltpu.make_async_copy(
            x_hbm.at[:, :, pl.ds(128 * t, 128)], s0.at[:, t, pl.ds(PAD, n), :], sems.at[t]
        )
        for t in range(m // 128)
    ]
    for copy in near + whole:
        copy.start()
    left = jnp.where(col == 0, 1.0, 0.0).astype(F32)
    right = jnp.where(col == counts[1] - 1, 1.0, 0.0).astype(F32)
    fill_blocks(mats, left, right)
    rim_mat[...] = rim_matrix(left, right)
    end_mat[...] = last_matrix(end_mat.shape[1], left, right)
    matrices = [mats.at[i] for i in range(4)] + [rim_mat]
    s0[:, :, 0:PAD, :] = jnp.zeros(s0.shape[:2] + (PAD, 128), F32)
    s0[:, :, PAD + n:, :] = jnp.zeros(s0.shape[:2] + (TAIL, 128), F32)
    down[...] = jnp.zeros_like(down)
    up[...] = jnp.zeros_like(up)
    strides = [64, 40, 40, 40]
    for ref, stride, filled in zip((e0, e1, e2, e3), strides, (48, 24, 16, 16)):
        for b in range(bands):
            ref[:, stride * b:stride * b + 8, :] = jnp.zeros((ref.shape[0], 8, 128), F32)
            rest = stride - 8 - filled
            ref[:, stride * (b + 1) - rest:stride * (b + 1), :] = jnp.zeros((ref.shape[0], rest, 128), F32)
    for copy in near:
        copy.wait()
    for b in range(bands):
        for t in range(m // 128):
            e0[t, 64 * b + 8:64 * b + 56, :] = raw[b, :, 128 * t:128 * t + 128]
    lane0 = 0
    for k, ref in enumerate((e0, e1, e2, e3)):
        stride = strides[k]
        head, foot, size = ((4, 24, 16), (5, 17, 8), (5, 16, 8), (5, 16, 8))[k]

        def reduced(t, start, size):
            e = [ref[t, pl.ds(start + i, size, stride=2), :] for i in range(5)]
            return 0.0625 * (e[0] + e[4]) + 0.25 * (e[1] + e[3]) + 0.375 * e[2]

        tiles = [
            jnp.concatenate(
                [
                    part for b in range(bands) for part in (
                        reduced(t, stride * b + head, 8), reduced(t, stride * b + foot, size)
                    )
                ],
                0,
            )
            for t in range(ref.shape[0])
        ]
        if k < LEVELS - 1:
            tiles = columns(tiles, m >> k, matrices)
        else:
            tiles = [split_dot(jnp.concatenate(tiles, 1), end_mat[...])]
        held = 8 + size
        first, count = ((23, 1), (14, 2), (10, 2), (8, 2))[k]
        for t, tile in enumerate(tiles):
            wide = pl.ds(lane0, 128)
            for b in range(bands):
                if k < LEVELS - 1:
                    stride_after = strides[k + 1]
                    (e1, e2, e3)[k][t, stride_after * b + 8:stride_after * b + 8 + held, :] = tile[held * b:held * b + held]
                down[2 * b:2 * b + count, wide] = tile[held * b + first:held * b + first + count]
                up[2 * b:2 * b + 1, wide] = tile[held * b:held * b + 1]
            lane0 += 128
    lower_part = jnp.where(bottom, 0.0, down[...])
    upper_part = jnp.where(top, 0.0, up[...])
    even = (row & 1) == 0
    send_e[...] = jnp.where(even, lower_part, upper_part)
    send_o[...] = jnp.where(even, upper_part, lower_part)
    for copy in whole:
        copy.wait()
    for b in range(bands):
        close(s0.at[b], n, top, bottom)


def pyramid_kernel(
    shape, counts, s0, mats, rim_mat, end_mat, one, two, three, four, rim_a, rim_b, s1, s2, s3,
):
    bands, n, m = shape
    row = lax.axis_index("row")
    top, bottom = row == 0, row == counts[0] - 1
    matrices = [mats.at[i] for i in range(4)] + [rim_mat]
    fields, outs = [s0, s1, s2, s3], [one, two, three, four]
    for k in range(1, LEVELS):
        ref, extent = fields[k], n >> k
        ref[:, :, PAD + extent + 8:, :] = jnp.zeros(ref.shape[:2] + (TAIL - 8, 128), F32)
    rim_b[...] = jnp.zeros_like(rim_b)
    sub = iota((8, 128), 0)
    for k in range(LEVELS):
        extent, cols = n >> k, m >> k
        half = extent // 2
        for b in range(bands):
            if k:
                close(fields[k].at[b], extent, top, bottom)
            tiles = [rows(fields[k].at[b, t], extent) for t in range(fields[k].shape[1])]
            if k < LEVELS - 1:
                tiles = columns(tiles, cols, matrices)
            else:
                tiles = [split_dot(jnp.concatenate(tiles, 1), end_mat[...])]
            for t, tile in enumerate(tiles):
                body, tail = tile[:half], tile[half:]
                if k < LEVELS - 1:
                    after = fields[k + 1]
                    after[b, t, PAD:PAD + half, :] = body
                    after[b, t, 0:PAD, :] = jnp.where(sub == 7, tail, 0.0)
                    after[b, t, PAD + half:PAD + half + 8, :] = jnp.where(sub < 2, tail, 0.0)
                    if t < len(tiles) - 1:
                        outs[k][b, :, 128 * t:128 * t + 128] = body
            body = tiles[-1][:half]
            start = sum(n >> j for j in range(2, k + 1))
            if k == LEVELS - 1:
                four[b] = body[:, :cols // 2]
                body = jnp.where(iota(body.shape, 1) < 2, pltpu.roll(body, 128 - cols // 2, 1), body)
            if k == 0:
                rim_a[b] = body
            else:
                rim_b[b, start:start + half, :] = body


def from_rows(got_e, got_o):
    even = (lax.axis_index("row") & 1) == 0
    e, o = got_e[...], got_o[...]
    return jnp.where(even, o, e), jnp.where(even, e, o)


def upper(part, b):
    part = pltpu.roll(part, 8 - 2 * b, 0) if b else part
    return jnp.where(iota(part.shape, 0) < 2, part, 0.0)


def lower(part, b):
    part = pltpu.roll(part, 7 - 2 * b, 0)
    return jnp.where(iota(part.shape, 0) == 7, part, 0.0)


def segments(n):
    out, start = [], 0
    for k in range(2, LEVELS + 1):
        out.append((k, start, n >> k))
        start += n >> k
    return out


def rim_kernel(shape, counts, rim_a, rim_b, got_e, got_o, send_e, send_o, tile_a, tile_b):
    bands, n, m = shape
    above, below = from_rows(got_e, got_o)
    offsets, start = [], 0
    for k in range(1, LEVELS + 1):
        cols = m >> k
        offsets.append(start + (cols if cols >= 128 else 0))
        start += lanes_of(cols)

    def rim_of(part, k):
        part = part[:, offsets[k - 1]:offsets[k - 1] + 128]
        if (m >> k) < 128:
            part = jnp.where(iota(part.shape, 1) < 2, pltpu.roll(part, 128 - (m >> k), 1), part)
        return part

    sub = iota((16, 128), 0)
    to_right, to_left = jnp.zeros((16, 128), F32), jnp.zeros((16, 128), F32)
    for b in range(bands):
        half = n // 2
        tile_a[b] = rim_a[b]
        tile_b[b] = rim_b[b]
        for ref, k, first, size in [(tile_a, 1, 0, half)] + [(tile_b, k, s, z) for k, s, z in segments(n)]:
            ref[b, first:first + 8, :] += upper(rim_of(above, k), b)
            ref[b, first + size - 8:first + size, :] += lower(rim_of(below, k), b)
        a = jnp.transpose(tile_a[b])
        c = jnp.transpose(tile_b[b])
        to_right = jnp.where(sub == 4 * b, a[0:1], to_right)
        to_right = jnp.where(sub == 4 * b + 1, c[0:1], to_right)
        to_right = jnp.where(sub == 4 * b + 2, c[1:2], to_right)
        to_left = jnp.where(sub == 4 * b, a[127:128], to_left)
        to_left = jnp.where(sub == 4 * b + 1, c[127:128], to_left)
    col = lax.axis_index("col")
    to_right = jnp.where(col == counts[1] - 1, 0.0, to_right)
    to_left = jnp.where(col == 0, 0.0, to_left)
    even = (col & 1) == 0
    send_e[...] = jnp.where(even, to_right, to_left)
    send_o[...] = jnp.where(even, to_left, to_right)


def finish_kernel(
    shape, one, two, three, four, row_e, row_o, col_e, col_o,
    out_one, out_two, out_three, out_four, tile_a, tile_b,
):
    bands, n, m = shape
    above, below = from_rows(row_e, row_o)
    even = (lax.axis_index("col") & 1) == 0
    before = jnp.where(even, col_o[...], col_e[...])
    after = jnp.where(even, col_e[...], col_o[...])
    fields, outs = [one, two, three, four], [out_one, out_two, out_three, out_four]
    tile_a[...] = jnp.zeros_like(tile_a)
    tile_b[...] = jnp.zeros_like(tile_b)
    lane = iota((128, 128), 1)
    for b in range(bands):
        tile_a[b, 0:1, :] = before[4 * b:4 * b + 1]
        tile_a[b, 127:128, :] = after[4 * b:4 * b + 1]
        tile_b[b, 0:2, :] = before[4 * b + 1:4 * b + 3]
        tile_b[b, 127:128, :] = after[4 * b + 1:4 * b + 2]
        tile_b[b, 63:64, :] = after[4 * b + 1:4 * b + 2]
        a = jnp.transpose(tile_a[b])
        c = jnp.transpose(tile_b[b])
        start = 0
        for k, first, size in [(1, 0, n // 2)] + segments(n):
            cols = m >> k
            part = (a if k == 1 else c)[first:first + size]
            wide = min(cols, 128)
            spot = lane[:size, :wide]
            part = part[:, :wide]
            low, high = jnp.where(spot < 2, part, 0.0), jnp.where(spot == wide - 1, part, 0.0)
            for t in range(cols // wide):
                at = pl.ds(wide * t, wide)
                value = fields[k - 1][b, :, at]
                if t == 0:
                    value = value + low
                if t == cols // wide - 1:
                    value = value + high
                outs[k - 1][b, :, at] = value
            top = upper(above[:, start:start + cols], b)
            end = lower(below[:, start:start + cols], b)
            outs[k - 1][b, 0:8, :] += top
            outs[k - 1][b, size - 8:size, :] += end
            start += lanes_of(cols)


def swap(pair, axis, counts):
    sizes = [counts[name] for name in ("row", "col")]
    along = ("row", "col").index(axis)
    out = []
    for parity, value in enumerate(pair):
        moves = []
        for i in range(sizes[0] * sizes[1]):
            place = list(divmod(i, sizes[1]))
            step = 1 if place[along] % 2 == parity else -1
            target = list(place)
            if 0 <= place[along] + step < sizes[along]:
                target[along] += step
            elif (place[1 - along] ^ 1) < sizes[1 - along]:
                target[1 - along] ^= 1
            else:
                continue
            moves.append((i, target[0] * sizes[1] + target[1]))
        out.append(lax.ppermute(value, ("row", "col"), moves))
    return out


def solution(mesh):
    counts = (mesh.shape["row"], mesh.shape["col"])

    def local(relief):
        shape = bands, n, m = relief.shape
        levels = [jax.ShapeDtypeStruct((bands, n >> k, m >> k), F32) for k in range(1, LEVELS + 1)]
        width = sum(lanes_of(m >> k) for k in range(1, LEVELS + 1))
        row_part = jax.ShapeDtypeStruct((8, width), F32)
        col_part = jax.ShapeDtypeStruct((16, 128), F32)
        rim = jax.ShapeDtypeStruct((bands, 128, 128), F32)
        tall = [
            jax.ShapeDtypeStruct((bands, (lanes_of(m >> k) if k else m) // 128, PAD + (n >> k) + TAIL, 128), F32)
            for k in range(LEVELS)
        ]
        send_e, send_o, field, *mats = pl.pallas_call(
            functools.partial(edge_kernel, shape, counts),
            out_shape=[
                row_part, row_part, tall[0],
                jax.ShapeDtypeStruct((4, 256, 256), BF16),
                jax.ShapeDtypeStruct((128, 256), BF16),
                jax.ShapeDtypeStruct((m >> 2, m >> 3), BF16),
            ],
            in_specs=[pl.BlockSpec(memory_space=pltpu.HBM)],
            out_specs=[VMEM] * 6,
            scratch_shapes=[
                pltpu.VMEM((bands, HEAD + FOOT, m), F32),
                pltpu.VMEM((m // 128, bands * 64, 128), F32),
            ] + [
                pltpu.VMEM((lanes_of(m >> k) // 128, bands * 40, 128), F32) for k in range(1, LEVELS)
            ] + [
                pltpu.VMEM((8, width), F32),
                pltpu.VMEM((8, width), F32),
                pltpu.SemaphoreType.DMA((2,)),
                pltpu.SemaphoreType.DMA((m // 128,)),
            ],
            compiler_params=pltpu.CompilerParams(vmem_limit_bytes=LIMIT),
            name="edge",
        )(pltpu.with_memory_space_constraint(relief, pltpu.HBM))
        *own, rim_a, rim_b = pl.pallas_call(
            functools.partial(pyramid_kernel, shape, counts),
            out_shape=levels + [rim, rim],
            in_specs=[VMEM] * 4,
            out_specs=[VMEM] * 6,
            scratch_shapes=[pltpu.VMEM(t.shape, F32) for t in tall[1:]],
            compiler_params=pltpu.CompilerParams(vmem_limit_bytes=LIMIT),
            cost_estimate=pl.CostEstimate(flops=8_000_000_000, bytes_accessed=0, transcendentals=0),
            name="pyramid",
        )(field, *mats)
        row_e, row_o = swap((send_e, send_o), "row", mesh.shape)
        send_e, send_o = pl.pallas_call(
            functools.partial(rim_kernel, shape, counts),
            out_shape=[col_part, col_part],
            in_specs=[VMEM] * 4,
            out_specs=[VMEM] * 2,
            scratch_shapes=[pltpu.VMEM((bands, 128, 128), F32)] * 2,
            compiler_params=pltpu.CompilerParams(vmem_limit_bytes=4 << 20),
            name="rim",
        )(rim_a, rim_b, row_e, row_o)
        col_e, col_o = swap((send_e, send_o), "col", mesh.shape)
        return tuple(pl.pallas_call(
            functools.partial(finish_kernel, shape),
            out_shape=levels,
            in_specs=[VMEM] * 8,
            out_specs=[VMEM] * 4,
            scratch_shapes=[pltpu.VMEM((bands, 128, 128), F32)] * 2,
            compiler_params=pltpu.CompilerParams(vmem_limit_bytes=8 << 20),
            name="finish",
        )(*own, row_e, row_o, col_e, col_o))

    placed = P(None, "row", "col")
    return jax.shard_map(
        local, mesh=mesh, in_specs=(placed,), out_specs=(placed,) * LEVELS, check_vma=False
    )
```

```python
import functools

import jax
import jax.numpy as jnp
from jax import lax
from jax.experimental import pallas as pl
from jax.experimental.pallas import tpu as pltpu
from jax.sharding import PartitionSpec as P


F32 = jnp.float32
BF16 = jnp.bfloat16
FAR = 1 << 20
LEVELS = 4
LIMIT = 24_000_000
VMEM = pl.BlockSpec(memory_space=pltpu.VMEM)
PAD = 8
TAIL = 24


def lanes_of(cols):
    return (cols + 3 + 127) // 128 * 128


def iota(shape, dim):
    return lax.broadcasted_iota(jnp.int32, shape, dim)


def band(source, target):
    far = jnp.abs(source - 2 * target)
    return jnp.where(far == 0, 0.375, jnp.where(far == 1, 0.25, jnp.where(far == 2, 0.0625, 0.0))).astype(F32)


def fill_blocks(mats, first, last):
    source, lane = iota((256, 256), 0), iota((256, 256), 1)
    target = jnp.where(lane <= 128, lane, jnp.where(lane == 255, -1, FAR))
    value = band(source, target)
    inside = value.astype(BF16)
    for i in range(4):
        mats[i] = inside
    source, target = iota((16, 128), 0), iota((16, 128), 1)
    mirror = jnp.where(source >= 1, band(-source, target), 0.0)
    start = (value[:16, :128] + first * mirror).astype(BF16)
    source = source + 240
    mirror = jnp.where(source == 254, band(source + 2, target), 0.0)
    end = (value[240:, :128] + last * mirror).astype(BF16)
    for i in (1, 3):
        mats[i, :16, :128] = start
    for i in (2, 3):
        mats[i, 240:, :128] = end


def rim_matrix(first, last):
    source, lane = iota((128, 256), 0), iota((128, 256), 1)
    after = source < 64
    col = jnp.where(after, 512 + source, source - 128)
    own = jnp.where(lane < 2, 256 + lane, jnp.where(lane == 127, -1, FAR))
    other = jnp.where(lane == 128, 0, jnp.where(lane == 255, 255, FAR))
    value = band(col, jnp.where(lane < 128, own, other))
    keep = jnp.where(after, 1.0 - last, 1.0 - first)
    return (value * keep).astype(BF16)


def last_matrix(cols, first, last):
    source, lane = iota((2 * cols, cols), 0), iota((2 * cols, cols), 1)
    half = cols // 2
    col = jnp.where(source < cols + cols // 2, source, source - 2 * cols)
    target = jnp.where(lane < half + 2, lane, jnp.where(lane == cols - 1, -1, FAR))
    value = band(col, target)
    value += first * jnp.where((source >= 1) & (source < cols), band(-source, target), 0.0)
    value += last * jnp.where(source == cols - 2, band(source + 2, target), 0.0)
    keep = jnp.where(col < 0, 1.0 - first, jnp.where(col >= cols, 1.0 - last, 1.0))
    return (value * keep).astype(BF16)


def split_dot(value, matrix):
    high = value.astype(BF16)
    low = (value - high.astype(F32)).astype(BF16)
    return (
        jnp.dot(high, matrix, preferred_element_type=F32)
        + jnp.dot(low, matrix, preferred_element_type=F32)
    )


def columns(tiles, cols, matrices):
    blocks = cols // 256
    rim = len(tiles) > 2 * blocks
    parts = []
    for t in range(blocks):
        index = (1 if t == 0 else 0) + (2 if t == blocks - 1 else 0)
        value = jnp.concatenate(tiles[2 * t:2 * t + 2], 1)
        parts.append(split_dot(value, matrices[index][...]))
    near = iota((tiles[0].shape[0], 128), 1) < 64
    edges = [p[:, 128:] for p in parts]
    if rim:
        around = split_dot(tiles[-1], matrices[4][...])
        edges.append(around[:, 128:])
    else:
        edges.append(jnp.zeros_like(edges[0]))
    out = [
        parts[t][:, :128] + jnp.where(near, edges[t - 1], edges[t + 1])
        for t in range(blocks)
    ]
    outer = jnp.where(near, edges[blocks - 1], edges[0])
    if rim:
        outer = outer + around[:, :128]
    return out + [outer]


def rows(ref, extent):
    half = extent // 2

    def reduced(start, size):
        e = [ref[pl.ds(start + t, size, stride=2), :] for t in range(5)]
        return 0.0625 * (e[0] + e[4]) + 0.25 * (e[1] + e[3]) + 0.375 * e[2]

    main = reduced(PAD - 2, half)
    below = reduced(PAD - 2 + extent, 8)
    above = 0.25 * ref[PAD - 1:PAD, :] + 0.0625 * ref[PAD:PAD + 1, :]
    return jnp.concatenate([main, jnp.where(iota(below.shape, 0) == 7, above, below)], 0)


def close(ref, extent, first, last):
    @pl.when(first)
    def _():
        ref[:, PAD - 2:PAD - 1, :] = ref[:, PAD + 2:PAD + 3, :]
        ref[:, PAD - 1:PAD, :] = ref[:, PAD + 1:PAD + 2, :]

    @pl.when(last)
    def _():
        ref[:, PAD + extent:PAD + extent + 1, :] = ref[:, PAD + extent - 2:PAD + extent - 1, :]


HEAD, FOOT = 16, 32


def edge_kernel(
    shape, counts, x_hbm, send_e, send_o, s0, mats, rim_mat, end_mat,
    raw, e0, e1, e2, e3, down, up, edge_sems, sems,
):
    bands, n, m = shape
    row, col = lax.axis_index("row"), lax.axis_index("col")
    top, bottom = row == 0, row == counts[0] - 1
    near = [
        pltpu.make_async_copy(x_hbm.at[:, pl.ds(0, HEAD), :], raw.at[:, pl.ds(0, HEAD), :], edge_sems.at[0]),
        pltpu.make_async_copy(x_hbm.at[:, pl.ds(n - FOOT, FOOT), :], raw.at[:, pl.ds(HEAD, FOOT), :], edge_sems.at[1]),
    ]
    whole = [
        pltpu.make_async_copy(
            x_hbm.at[:, :, pl.ds(128 * t, 128)], s0.at[:, t, pl.ds(PAD, n), :], sems.at[t]
        )
        for t in range(m // 128)
    ]
    for copy in near + whole:
        copy.start()
    left = jnp.where(col == 0, 1.0, 0.0).astype(F32)
    right = jnp.where(col == counts[1] - 1, 1.0, 0.0).astype(F32)
    fill_blocks(mats, left, right)
    rim_mat[...] = rim_matrix(left, right)
    end_mat[...] = last_matrix(end_mat.shape[1], left, right)
    matrices = [mats.at[i] for i in range(4)] + [rim_mat]
    s0[:, :, 0:PAD, :] = jnp.zeros(s0.shape[:2] + (PAD, 128), F32)
    s0[:, :, PAD + n:, :] = jnp.zeros(s0.shape[:2] + (TAIL, 128), F32)
    down[...] = jnp.zeros_like(down)
    up[...] = jnp.zeros_like(up)
    strides = [64, 40, 40, 40]
    for ref, stride, filled in zip((e0, e1, e2, e3), strides, (48, 24, 16, 16)):
        for b in range(bands):
            ref[:, stride * b:stride * b + 8, :] = jnp.zeros((ref.shape[0], 8, 128), F32)
            rest = stride - 8 - filled
            ref[:, stride * (b + 1) - rest:stride * (b + 1), :] = jnp.zeros((ref.shape[0], rest, 128), F32)
    for copy in near:
        copy.wait()
    for b in range(bands):
        for t in range(m // 128):
            e0[t, 64 * b + 8:64 * b + 56, :] = raw[b, :, 128 * t:128 * t + 128]
    lane0 = 0
    for k, ref in enumerate((e0, e1, e2, e3)):
        stride = strides[k]
        head, foot, size = ((4, 24, 16), (5, 17, 8), (5, 16, 8), (5, 16, 8))[k]

        def reduced(t, start, size):
            e = [ref[t, pl.ds(start + i, size, stride=2), :] for i in range(5)]
            return 0.0625 * (e[0] + e[4]) + 0.25 * (e[1] + e[3]) + 0.375 * e[2]

        tiles = [
            jnp.concatenate(
                [
                    part for b in range(bands) for part in (
                        reduced(t, stride * b + head, 8), reduced(t, stride * b + foot, size)
                    )
                ],
                0,
            )
            for t in range(ref.shape[0])
        ]
        if k < LEVELS - 1:
            tiles = columns(tiles, m >> k, matrices)
        else:
            tiles = [split_dot(jnp.concatenate(tiles, 1), end_mat[...])]
        held = 8 + size
        first, count = ((23, 1), (14, 2), (10, 2), (8, 2))[k]
        for t, tile in enumerate(tiles):
            wide = pl.ds(lane0, 128)
            for b in range(bands):
                if k < LEVELS - 1:
                    stride_after = strides[k + 1]
                    (e1, e2, e3)[k][t, stride_after * b + 8:stride_after * b + 8 + held, :] = tile[held * b:held * b + held]
                down[2 * b:2 * b + count, wide] = tile[held * b + first:held * b + first + count]
                up[2 * b:2 * b + 1, wide] = tile[held * b:held * b + 1]
            lane0 += 128
    lower_part = jnp.where(bottom, 0.0, down[...])
    upper_part = jnp.where(top, 0.0, up[...])
    even = (row & 1) == 0
    send_e[...] = jnp.where(even, lower_part, upper_part)
    send_o[...] = jnp.where(even, upper_part, lower_part)
    for copy in whole:
        copy.wait()
    for b in range(bands):
        close(s0.at[b], n, top, bottom)


def pyramid_kernel(
    shape, counts, s0, mats, rim_mat, end_mat, one, two, three, four, rim_a, rim_b, s1, s2, s3,
):
    bands, n, m = shape
    row = lax.axis_index("row")
    top, bottom = row == 0, row == counts[0] - 1
    matrices = [mats.at[i] for i in range(4)] + [rim_mat]
    fields, outs = [s0, s1, s2, s3], [one, two, three, four]
    sub = iota((8, 128), 0)

    def store(k, b, t, tile):
        half = n >> (k + 1)
        tail, after = tile[half:], fields[k + 1]
        after[b, t, PAD:PAD + half, :] = tile[:half]
        after[b, t, 0:PAD, :] = jnp.where(sub == 7, tail, 0.0)
        after[b, t, PAD + half:PAD + half + 8, :] = jnp.where(sub < 2, tail, 0.0)
        after[b, t, PAD + half + 8:, :] = jnp.zeros((TAIL - 8, 128), F32)
        if 128 * t < outs[k].shape[2]:
            outs[k][b, :, 128 * t:128 * t + 128] = tile[:half]
        elif k == 0:
            rim_a[b] = tile[:half]

    def level_one(b, _):
        tiles = columns([rows(s0.at[b, t], n) for t in range(m // 128)], m, matrices)
        for t, tile in enumerate(tiles):
            store(0, b, t, tile)
        return 0

    lax.fori_loop(0, bands, level_one, 0)
    start = 0
    for k in range(1, LEVELS):
        extent, cols = n >> k, m >> k
        half = extent // 2
        for b in range(bands):
            close(fields[k].at[b], extent, top, bottom)
        tiles = [
            jnp.concatenate([rows(fields[k].at[b, t], extent) for b in range(bands)], 0)
            for t in range(fields[k].shape[1])
        ]
        if k < LEVELS - 1:
            tiles = columns(tiles, cols, matrices)
        else:
            tiles = [split_dot(jnp.concatenate(tiles, 1), end_mat[...])]
        for b in range(bands):
            parts = [tile[(half + 8) * b:(half + 8) * (b + 1)] for tile in tiles]
            body = parts[-1][:half]
            if k < LEVELS - 1:
                for t, tile in enumerate(parts):
                    store(k, b, t, tile)
            else:
                four[b] = body[:, :cols // 2]
                body = jnp.where(iota(body.shape, 1) < 2, pltpu.roll(body, 128 - cols // 2, 1), body)
            rim_b[b, start:start + half, :] = body
        start += half
    rim_b[:, start:, :] = jnp.zeros((bands, 128 - start, 128), F32)


def from_rows(got_e, got_o):
    even = (lax.axis_index("row") & 1) == 0
    e, o = got_e[...], got_o[...]
    return jnp.where(even, o, e), jnp.where(even, e, o)


def upper(part, b):
    part = pltpu.roll(part, 8 - 2 * b, 0) if b else part
    return jnp.where(iota(part.shape, 0) < 2, part, 0.0)


def lower(part, b):
    part = pltpu.roll(part, 7 - 2 * b, 0)
    return jnp.where(iota(part.shape, 0) == 7, part, 0.0)


def segments(n):
    out, start = [], 0
    for k in range(2, LEVELS + 1):
        out.append((k, start, n >> k))
        start += n >> k
    return out


def rim_kernel(
    shape, counts, rim_a, rim_b, got_e, got_o, send_0, send_1, send_2, tile_a, tile_b
):
    bands, n, m = shape
    above, below = from_rows(got_e, got_o)
    offsets, start = [], 0
    for k in range(1, LEVELS + 1):
        cols = m >> k
        offsets.append(start + (cols if cols >= 128 else 0))
        start += lanes_of(cols)

    def rim_of(part, k):
        part = part[:, offsets[k - 1]:offsets[k - 1] + 128]
        if (m >> k) < 128:
            part = jnp.where(iota(part.shape, 1) < 2, pltpu.roll(part, 128 - (m >> k), 1), part)
        return part

    sub = iota((16, 128), 0)
    to_right, to_left = jnp.zeros((16, 128), F32), jnp.zeros((16, 128), F32)
    for b in range(bands):
        half = n // 2
        tile_a[b] = rim_a[b]
        tile_b[b] = rim_b[b]
        for ref, k, first, size in [(tile_a, 1, 0, half)] + [(tile_b, k, s, z) for k, s, z in segments(n)]:
            ref[b, first:first + 8, :] += upper(rim_of(above, k), b)
            ref[b, first + size - 8:first + size, :] += lower(rim_of(below, k), b)
        a = jnp.transpose(tile_a[b])
        c = jnp.transpose(tile_b[b])
        to_right = jnp.where(sub == 4 * b, a[0:1], to_right)
        to_right = jnp.where(sub == 4 * b + 1, c[0:1], to_right)
        to_right = jnp.where(sub == 4 * b + 2, c[1:2], to_right)
        to_left = jnp.where(sub == 4 * b, a[127:128], to_left)
        to_left = jnp.where(sub == 4 * b + 1, c[127:128], to_left)
    col = lax.axis_index("col")
    to_right = jnp.where(col == counts[1] - 1, 0.0, to_right)
    to_left = jnp.where(col == 0, 0.0, to_left)
    for k, send in enumerate((send_0, send_1, send_2)):
        left = jnp.where((col + 2) % 3 == k, to_left, 0.0)
        send[...] = jnp.where(col % 3 == k, to_right, left)


def finish_kernel(
    shape, one, two, three, four, row_e, row_o, col_0, col_1, col_2,
    out_one, out_two, out_three, out_four, tile_a, tile_b,
):
    bands, n, m = shape
    above, below = from_rows(row_e, row_o)
    turn = lax.axis_index("col") % 3
    got = [col_0[...], col_1[...], col_2[...]]
    after = jnp.where(turn == 0, got[0], jnp.where(turn == 1, got[1], got[2]))
    before = jnp.where(turn == 0, got[2], jnp.where(turn == 1, got[0], got[1]))
    fields, outs = [one, two, three, four], [out_one, out_two, out_three, out_four]
    tile_a[...] = jnp.zeros_like(tile_a)
    tile_b[...] = jnp.zeros_like(tile_b)
    lane = iota((128, 128), 1)
    for b in range(bands):
        tile_a[b, 0:1, :] = before[4 * b:4 * b + 1]
        tile_a[b, 127:128, :] = after[4 * b:4 * b + 1]
        tile_b[b, 0:2, :] = before[4 * b + 1:4 * b + 3]
        tile_b[b, 127:128, :] = after[4 * b + 1:4 * b + 2]
        tile_b[b, 63:64, :] = after[4 * b + 1:4 * b + 2]
        a = jnp.transpose(tile_a[b])
        c = jnp.transpose(tile_b[b])
        start = 0
        for k, first, size in [(1, 0, n // 2)] + segments(n):
            cols = m >> k
            part = (a if k == 1 else c)[first:first + size]
            wide = min(cols, 128)
            spot = lane[:size, :wide]
            part = part[:, :wide]
            low, high = jnp.where(spot < 2, part, 0.0), jnp.where(spot == wide - 1, part, 0.0)
            for t in range(cols // wide):
                at = pl.ds(wide * t, wide)
                value = fields[k - 1][b, :, at]
                if t == 0:
                    value = value + low
                if t == cols // wide - 1:
                    value = value + high
                outs[k - 1][b, :, at] = value
            top = upper(above[:, start:start + cols], b)
            end = lower(below[:, start:start + cols], b)
            outs[k - 1][b, 0:8, :] += top
            outs[k - 1][b, size - 8:size, :] += end
            start += lanes_of(cols)


def swap(values, axis, counts):
    sizes = [counts[name] for name in ("row", "col")]
    along = ("row", "col").index(axis)
    out = []
    for k, value in enumerate(values):
        moves = []
        for i in range(sizes[0] * sizes[1]):
            place = list(divmod(i, sizes[1]))
            target = list(place)
            here = place[along]
            if here % len(values) == k and here + 1 < sizes[along]:
                target[along] += 1
            elif (here - 1) % len(values) == k and here > 0:
                target[along] -= 1
            elif (place[1 - along] ^ 1) < sizes[1 - along]:
                target[1 - along] ^= 1
            else:
                continue
            moves.append((i, target[0] * sizes[1] + target[1]))
        out.append(lax.ppermute(value, ("row", "col"), moves))
    return out


def solution(mesh):
    counts = (mesh.shape["row"], mesh.shape["col"])

    def local(relief):
        shape = bands, n, m = relief.shape
        levels = [jax.ShapeDtypeStruct((bands, n >> k, m >> k), F32) for k in range(1, LEVELS + 1)]
        width = sum(lanes_of(m >> k) for k in range(1, LEVELS + 1))
        row_part = jax.ShapeDtypeStruct((8, width), F32)
        col_part = jax.ShapeDtypeStruct((16, 128), F32)
        rim = jax.ShapeDtypeStruct((bands, 128, 128), F32)
        tall = [
            jax.ShapeDtypeStruct((bands, (lanes_of(m >> k) if k else m) // 128, PAD + (n >> k) + TAIL, 128), F32)
            for k in range(LEVELS)
        ]
        send_e, send_o, field, *mats = pl.pallas_call(
            functools.partial(edge_kernel, shape, counts),
            out_shape=[
                row_part, row_part, tall[0],
                jax.ShapeDtypeStruct((4, 256, 256), BF16),
                jax.ShapeDtypeStruct((128, 256), BF16),
                jax.ShapeDtypeStruct((m >> 2, m >> 3), BF16),
            ],
            in_specs=[pl.BlockSpec(memory_space=pltpu.HBM)],
            out_specs=[VMEM] * 6,
            scratch_shapes=[
                pltpu.VMEM((bands, HEAD + FOOT, m), F32),
                pltpu.VMEM((m // 128, bands * 64, 128), F32),
            ] + [
                pltpu.VMEM((lanes_of(m >> k) // 128, bands * 40, 128), F32) for k in range(1, LEVELS)
            ] + [
                pltpu.VMEM((8, width), F32),
                pltpu.VMEM((8, width), F32),
                pltpu.SemaphoreType.DMA((2,)),
                pltpu.SemaphoreType.DMA((m // 128,)),
            ],
            compiler_params=pltpu.CompilerParams(vmem_limit_bytes=LIMIT),
            name="edge",
        )(pltpu.with_memory_space_constraint(relief, pltpu.HBM))
        *own, rim_a, rim_b = pl.pallas_call(
            functools.partial(pyramid_kernel, shape, counts),
            out_shape=levels + [rim, rim],
            in_specs=[VMEM] * 4,
            out_specs=[VMEM] * 6,
            scratch_shapes=[pltpu.VMEM(t.shape, F32) for t in tall[1:]],
            compiler_params=pltpu.CompilerParams(vmem_limit_bytes=LIMIT),
            cost_estimate=pl.CostEstimate(flops=8_000_000_000, bytes_accessed=0, transcendentals=0),
            name="pyramid",
        )(field, *mats)
        row_e, row_o = swap((send_e, send_o), "row", mesh.shape)
        sends = pl.pallas_call(
            functools.partial(rim_kernel, shape, counts),
            out_shape=[col_part] * 3,
            in_specs=[VMEM] * 4,
            out_specs=[VMEM] * 3,
            scratch_shapes=[pltpu.VMEM((bands, 128, 128), F32)] * 2,
            compiler_params=pltpu.CompilerParams(vmem_limit_bytes=4 << 20),
            name="rim",
        )(rim_a, rim_b, row_e, row_o)
        cols = swap(sends, "col", mesh.shape)
        return tuple(pl.pallas_call(
            functools.partial(finish_kernel, shape),
            out_shape=levels,
            in_specs=[VMEM] * 9,
            out_specs=[VMEM] * 4,
            scratch_shapes=[pltpu.VMEM((bands, 128, 128), F32)] * 2,
            compiler_params=pltpu.CompilerParams(vmem_limit_bytes=8 << 20),
            name="finish",
        )(*own, row_e, row_o, *cols))

    placed = P(None, "row", "col")
    return jax.shard_map(
        local, mesh=mesh, in_specs=(placed,), out_specs=(placed,) * LEVELS, check_vma=False
    )
```

```python
import functools

import jax
import jax.numpy as jnp
from jax import lax
from jax.experimental import pallas as pl
from jax.experimental.pallas import tpu as pltpu
from jax.sharding import PartitionSpec as P


F32 = jnp.float32
BF16 = jnp.bfloat16
FAR = 1 << 20
LEVELS = 4
LIMIT = 24_000_000
VMEM = pl.BlockSpec(memory_space=pltpu.VMEM)
PAD = 8
TAIL = 24


def lanes_of(cols):
    return (cols + 3 + 127) // 128 * 128


def iota(shape, dim):
    return lax.broadcasted_iota(jnp.int32, shape, dim)


def band(source, target):
    far = jnp.abs(source - 2 * target)
    return jnp.where(far == 0, 0.375, jnp.where(far == 1, 0.25, jnp.where(far == 2, 0.0625, 0.0))).astype(F32)


def fill_blocks(mats, first, last):
    source, lane = iota((256, 256), 0), iota((256, 256), 1)
    target = jnp.where(lane <= 128, lane, jnp.where(lane == 255, -1, FAR))
    value = band(source, target)
    inside = value.astype(BF16)
    for i in range(4):
        mats[i] = inside
    source, target = iota((16, 128), 0), iota((16, 128), 1)
    mirror = jnp.where(source >= 1, band(-source, target), 0.0)
    start = (value[:16, :128] + first * mirror).astype(BF16)
    source = source + 240
    mirror = jnp.where(source == 254, band(source + 2, target), 0.0)
    end = (value[240:, :128] + last * mirror).astype(BF16)
    for i in (1, 3):
        mats[i, :16, :128] = start
    for i in (2, 3):
        mats[i, 240:, :128] = end


def rim_matrix(first, last):
    source, lane = iota((128, 256), 0), iota((128, 256), 1)
    after = source < 64
    col = jnp.where(after, 512 + source, source - 128)
    own = jnp.where(lane < 2, 256 + lane, jnp.where(lane == 127, -1, FAR))
    other = jnp.where(lane == 128, 0, jnp.where(lane == 255, 255, FAR))
    value = band(col, jnp.where(lane < 128, own, other))
    keep = jnp.where(after, 1.0 - last, 1.0 - first)
    return (value * keep).astype(BF16)


def last_matrix(cols, first, last):
    source, lane = iota((2 * cols, cols), 0), iota((2 * cols, cols), 1)
    half = cols // 2
    col = jnp.where(source < cols + cols // 2, source, source - 2 * cols)
    target = jnp.where(lane < half + 2, lane, jnp.where(lane == cols - 1, -1, FAR))
    value = band(col, target)
    value += first * jnp.where((source >= 1) & (source < cols), band(-source, target), 0.0)
    value += last * jnp.where(source == cols - 2, band(source + 2, target), 0.0)
    keep = jnp.where(col < 0, 1.0 - first, jnp.where(col >= cols, 1.0 - last, 1.0))
    return (value * keep).astype(BF16)


def split_dot(value, matrix):
    high = value.astype(BF16)
    low = (value - high.astype(F32)).astype(BF16)
    return (
        jnp.dot(high, matrix, preferred_element_type=F32)
        + jnp.dot(low, matrix, preferred_element_type=F32)
    )


def columns(tiles, cols, matrices):
    blocks = cols // 256
    rim = len(tiles) > 2 * blocks
    parts = []
    for t in range(blocks):
        index = (1 if t == 0 else 0) + (2 if t == blocks - 1 else 0)
        value = jnp.concatenate(tiles[2 * t:2 * t + 2], 1)
        parts.append(split_dot(value, matrices[index][...]))
    near = iota((tiles[0].shape[0], 128), 1) < 64
    edges = [p[:, 128:] for p in parts]
    if rim:
        around = split_dot(tiles[-1], matrices[4][...])
        edges.append(around[:, 128:])
    else:
        edges.append(jnp.zeros_like(edges[0]))
    out = [
        parts[t][:, :128] + jnp.where(near, edges[t - 1], edges[t + 1])
        for t in range(blocks)
    ]
    outer = jnp.where(near, edges[blocks - 1], edges[0])
    if rim:
        outer = outer + around[:, :128]
    return out + [outer]


def rows(ref, extent):
    half = extent // 2

    def reduced(start, size):
        e = [ref[pl.ds(start + t, size, stride=2), :] for t in range(5)]
        return 0.0625 * (e[0] + e[4]) + 0.25 * (e[1] + e[3]) + 0.375 * e[2]

    main = reduced(PAD - 2, half)
    below = reduced(PAD - 2 + extent, 8)
    above = 0.25 * ref[PAD - 1:PAD, :] + 0.0625 * ref[PAD:PAD + 1, :]
    return jnp.concatenate([main, jnp.where(iota(below.shape, 0) == 7, above, below)], 0)


def close(ref, extent, first, last):
    @pl.when(first)
    def _():
        ref[:, PAD - 2:PAD - 1, :] = ref[:, PAD + 2:PAD + 3, :]
        ref[:, PAD - 1:PAD, :] = ref[:, PAD + 1:PAD + 2, :]

    @pl.when(last)
    def _():
        ref[:, PAD + extent:PAD + extent + 1, :] = ref[:, PAD + extent - 2:PAD + extent - 1, :]


def slots(bands, m):
    place, tiles = {}, 0
    for k in range(2, LEVELS + 1):
        for t in range(lanes_of(m >> k) // 128):
            for b in range(bands):
                place[k, t, b] = tiles, 2 * b
            tiles += 1
    free = [(j, r) for j in range(tiles) for r in range(2 * bands, 8)]
    for t in range(lanes_of(m >> 1) // 128):
        for b in range(bands):
            if not free:
                free = [(tiles, r) for r in range(8)]
                tiles += 1
            place[1, t, b] = free.pop(0)
    return place, tiles


HEAD, FOOT = 16, 32


def edge_kernel(
    shape, counts, x_hbm, send_e, send_o, s0, mats, rim_mat, end_mat,
    raw, e0, e1, e2, e3, down, up, edge_sems, sems,
):
    bands, n, m = shape
    row, col = lax.axis_index("row"), lax.axis_index("col")
    top, bottom = row == 0, row == counts[0] - 1
    near = [
        pltpu.make_async_copy(x_hbm.at[:, pl.ds(0, HEAD), :], raw.at[:, pl.ds(0, HEAD), :], edge_sems.at[0]),
        pltpu.make_async_copy(x_hbm.at[:, pl.ds(n - FOOT, FOOT), :], raw.at[:, pl.ds(HEAD, FOOT), :], edge_sems.at[1]),
    ]
    whole = [
        pltpu.make_async_copy(
            x_hbm.at[:, :, pl.ds(128 * t, 128)], s0.at[:, t, pl.ds(PAD, n), :], sems.at[t]
        )
        for t in range(m // 128)
    ]
    for copy in near + whole:
        copy.start()
    left = jnp.where(col == 0, 1.0, 0.0).astype(F32)
    right = jnp.where(col == counts[1] - 1, 1.0, 0.0).astype(F32)
    fill_blocks(mats, left, right)
    rim_mat[...] = rim_matrix(left, right)
    end_mat[...] = last_matrix(end_mat.shape[1], left, right)
    matrices = [mats.at[i] for i in range(4)] + [rim_mat]
    s0[:, :, 0:PAD, :] = jnp.zeros(s0.shape[:2] + (PAD, 128), F32)
    s0[:, :, PAD + n:, :] = jnp.zeros(s0.shape[:2] + (TAIL, 128), F32)
    down[...] = jnp.zeros_like(down)
    up[...] = jnp.zeros_like(up)
    strides = [64, 40, 40, 40]
    for ref, stride, filled in zip((e0, e1, e2, e3), strides, (48, 24, 16, 16)):
        for b in range(bands):
            ref[:, stride * b:stride * b + 8, :] = jnp.zeros((ref.shape[0], 8, 128), F32)
            rest = stride - 8 - filled
            ref[:, stride * (b + 1) - rest:stride * (b + 1), :] = jnp.zeros((ref.shape[0], rest, 128), F32)
    for copy in near:
        copy.wait()
    for b in range(bands):
        for t in range(m // 128):
            e0[t, 64 * b + 8:64 * b + 56, :] = raw[b, :, 128 * t:128 * t + 128]
    place, _ = slots(bands, m)
    for k, ref in enumerate((e0, e1, e2, e3)):
        stride = strides[k]
        head, foot, size = ((4, 24, 16), (5, 17, 8), (5, 16, 8), (5, 16, 8))[k]

        def reduced(t, start, size):
            e = [ref[t, pl.ds(start + i, size, stride=2), :] for i in range(5)]
            return 0.0625 * (e[0] + e[4]) + 0.25 * (e[1] + e[3]) + 0.375 * e[2]

        tiles = [
            jnp.concatenate(
                [
                    part for b in range(bands) for part in (
                        reduced(t, stride * b + head, 8), reduced(t, stride * b + foot, size)
                    )
                ],
                0,
            )
            for t in range(ref.shape[0])
        ]
        if k < LEVELS - 1:
            tiles = columns(tiles, m >> k, matrices)
        else:
            tiles = [split_dot(jnp.concatenate(tiles, 1), end_mat[...])]
        held = 8 + size
        first, count = ((23, 1), (14, 2), (10, 2), (8, 2))[k]
        for t, tile in enumerate(tiles):
            for b in range(bands):
                if k < LEVELS - 1:
                    stride_after = strides[k + 1]
                    (e1, e2, e3)[k][t, stride_after * b + 8:stride_after * b + 8 + held, :] = tile[held * b:held * b + held]
                spot, line = place[k + 1, t, b]
                wide = pl.ds(128 * spot, 128)
                down[line:line + count, wide] = tile[held * b + first:held * b + first + count]
                up[line:line + 1, wide] = tile[held * b:held * b + 1]
    lower_part = jnp.where(bottom, 0.0, down[...])
    upper_part = jnp.where(top, 0.0, up[...])
    even = (row & 1) == 0
    send_e[...] = jnp.where(even, lower_part, upper_part)
    send_o[...] = jnp.where(even, upper_part, lower_part)
    for copy in whole:
        copy.wait()
    for b in range(bands):
        close(s0.at[b], n, top, bottom)


def pyramid_kernel(
    shape, counts, s0, mats, rim_mat, end_mat, one, two, three, four, rim_a, rim_b, s1, s2, s3,
):
    bands, n, m = shape
    row = lax.axis_index("row")
    top, bottom = row == 0, row == counts[0] - 1
    matrices = [mats.at[i] for i in range(4)] + [rim_mat]
    fields, outs = [s0, s1, s2, s3], [one, two, three, four]
    sub = iota((8, 128), 0)

    def store(k, b, t, tile):
        half = n >> (k + 1)
        tail, after = tile[half:], fields[k + 1]
        after[b, t, PAD:PAD + half, :] = tile[:half]
        after[b, t, 0:PAD, :] = jnp.where(sub == 7, tail, 0.0)
        after[b, t, PAD + half:PAD + half + 8, :] = jnp.where(sub < 2, tail, 0.0)
        after[b, t, PAD + half + 8:, :] = jnp.zeros((TAIL - 8, 128), F32)
        if 128 * t < outs[k].shape[2]:
            outs[k][b, :, 128 * t:128 * t + 128] = tile[:half]
        elif k == 0:
            rim_a[b] = tile[:half]

    def level_one(b, _):
        tiles = columns([rows(s0.at[b, t], n) for t in range(m // 128)], m, matrices)
        for t, tile in enumerate(tiles):
            store(0, b, t, tile)
        return 0

    lax.fori_loop(0, bands, level_one, 0)
    start = 0
    for k in range(1, LEVELS):
        extent, cols = n >> k, m >> k
        half = extent // 2
        for b in range(bands):
            close(fields[k].at[b], extent, top, bottom)
        tiles = [
            jnp.concatenate([rows(fields[k].at[b, t], extent) for b in range(bands)], 0)
            for t in range(fields[k].shape[1])
        ]
        if k < LEVELS - 1:
            tiles = columns(tiles, cols, matrices)
        else:
            tiles = [split_dot(jnp.concatenate(tiles, 1), end_mat[...])]
        for b in range(bands):
            parts = [tile[(half + 8) * b:(half + 8) * (b + 1)] for tile in tiles]
            body = parts[-1][:half]
            if k < LEVELS - 1:
                for t, tile in enumerate(parts):
                    store(k, b, t, tile)
            else:
                four[b] = body[:, :cols // 2]
                body = jnp.where(iota(body.shape, 1) < 2, pltpu.roll(body, 128 - cols // 2, 1), body)
            rim_b[b, start:start + half, :] = body
        start += half
    rim_b[:, start:, :] = jnp.zeros((bands, 128 - start, 128), F32)


def from_rows(got_e, got_o):
    even = (lax.axis_index("row") & 1) == 0
    e, o = got_e[...], got_o[...]
    return jnp.where(even, o, e), jnp.where(even, e, o)


def row_parts(above, below, place, k, t, b):
    spot, line = place[k, t, b]
    head, foot = (part[:, 128 * spot:128 * spot + 128] for part in (above, below))
    sub = iota(head.shape, 0)
    head = pltpu.roll(head, 8 - line, 0) if line else head
    foot = pltpu.roll(foot, 7 - line, 0) if line < 7 else foot
    return jnp.where(sub < (1 if k == 1 else 2), head, 0.0), jnp.where(sub == 7, foot, 0.0)


def segments(n):
    out, start = [], 0
    for k in range(2, LEVELS + 1):
        out.append((k, start, n >> k))
        start += n >> k
    return out


def rim_kernel(
    shape, counts, rim_a, rim_b, got_e, got_o, send_0, send_1, send_2, tile_a, tile_b
):
    bands, n, m = shape
    above, below = from_rows(got_e, got_o)
    place, _ = slots(bands, m)

    def rim_of(k, b):
        parts = row_parts(above, below, place, k, (m >> k) // 128, b)
        if (m >> k) < 128:
            parts = [jnp.where(iota(p.shape, 1) < 2, pltpu.roll(p, 128 - (m >> k), 1), p) for p in parts]
        return parts

    sub = iota((16, 128), 0)
    to_right, to_left = jnp.zeros((16, 128), F32), jnp.zeros((16, 128), F32)
    for b in range(bands):
        half = n // 2
        tile_a[b] = rim_a[b]
        tile_b[b] = rim_b[b]
        for ref, k, first, size in [(tile_a, 1, 0, half)] + [(tile_b, k, s, z) for k, s, z in segments(n)]:
            head, foot = rim_of(k, b)
            ref[b, first:first + 8, :] += head
            ref[b, first + size - 8:first + size, :] += foot
        a = jnp.transpose(tile_a[b])
        c = jnp.transpose(tile_b[b])
        to_right = jnp.where(sub == 4 * b, a[0:1], to_right)
        to_right = jnp.where(sub == 4 * b + 1, c[0:1], to_right)
        to_right = jnp.where(sub == 4 * b + 2, c[1:2], to_right)
        to_left = jnp.where(sub == 4 * b, a[127:128], to_left)
        to_left = jnp.where(sub == 4 * b + 1, c[127:128], to_left)
    col = lax.axis_index("col")
    to_right = jnp.where(col == counts[1] - 1, 0.0, to_right)
    to_left = jnp.where(col == 0, 0.0, to_left)
    for k, send in enumerate((send_0, send_1, send_2)):
        left = jnp.where((col + 2) % 3 == k, to_left, 0.0)
        send[...] = jnp.where(col % 3 == k, to_right, left)


def settle_kernel(
    shape, one, two, three, four, row_e, row_o, out, done_one, done_two, done_three, done_four, inner, sems
):
    bands, n, m = shape
    above, below = from_rows(row_e, row_o)
    place, _ = slots(bands, m)
    tiles = (m >> 1) // 128
    copies = []
    for b in range(bands):
        for k, (field, done) in enumerate(zip((one, two, three, four), (done_one, done_two, done_three, done_four)), 1):
            cols, size = m >> k, n >> k
            wide = min(cols, 128)
            for t in range(cols // wide):
                at, to, ref = pl.ds(wide * t, wide), pl.ds(wide * t, wide), done
                if k == 1:
                    if 0 < t < tiles - 1:
                        ref, to = inner, pl.ds(128 * (t - 1), 128)
                    else:
                        to = pl.ds(128 * min(t, 1), 128)
                head, foot = row_parts(above, below, place, k, t, b)
                ref[b, 0:8, to] = field[b, 0:8, at] + head[:, :wide]
                if size > 16:
                    ref[b, 8:size - 8, to] = field[b, 8:size - 8, at]
                ref[b, size - 8:size, to] = field[b, size - 8:size, at] + foot[:, :wide]
            if k == 1:
                copy = pltpu.make_async_copy(
                    inner.at[b], out.at[b, :, pl.ds(128, 128 * (tiles - 2))], sems.at[b]
                )
                copy.start()
                copies.append(copy)
    for copy in copies:
        copy.wait()


def finish_kernel(
    shape, _, one, two, three, four, col_0, col_1, col_2,
    out_one, out_two, out_three, out_four, tile_a, tile_b, new_one, new_two, new_three, new_four, sems,
):
    bands, n, m = shape
    turn = lax.axis_index("col") % 3
    got = [col_0[...], col_1[...], col_2[...]]
    after = jnp.where(turn == 0, got[0], jnp.where(turn == 1, got[1], got[2]))
    before = jnp.where(turn == 0, got[2], jnp.where(turn == 1, got[0], got[1]))
    fields, news = [one, two, three, four], [new_one, new_two, new_three, new_four]
    outs = [out_one, out_two, out_three, out_four]
    tile_a[...] = jnp.zeros_like(tile_a)
    tile_b[...] = jnp.zeros_like(tile_b)
    lane = iota((128, 128), 1)
    copies = []

    def send(source, target):
        copy = pltpu.make_async_copy(source, target, sems.at[len(copies)])
        copy.start()
        copies.append(copy)

    def add(k, b, part):
        cols, size = m >> k, part.shape[0]
        wide = min(cols, 128)
        spot = lane[:size, :wide]
        part = part[:, :wide]
        low, high = jnp.where(spot < 2, part, 0.0), jnp.where(spot == wide - 1, part, 0.0)
        count = min(cols // wide, 2)
        for t in range(count):
            at = pl.ds(wide * t, wide)
            value = fields[k - 1][b, :, at]
            if t == 0:
                value = value + low
            if t == count - 1:
                value = value + high
            news[k - 1][b, :, at] = value

    for b in range(bands):
        tile_a[b, 0:1, :] = before[4 * b:4 * b + 1]
        tile_a[b, 127:128, :] = after[4 * b:4 * b + 1]
        tile_b[b, 0:2, :] = before[4 * b + 1:4 * b + 3]
        tile_b[b, 127:128, :] = after[4 * b + 1:4 * b + 2]
        tile_b[b, 63:64, :] = after[4 * b + 1:4 * b + 2]
    for b in range(bands):
        add(1, b, jnp.transpose(tile_a[b]))
        for t, at in enumerate((0, (m >> 1) - 128)):
            send(new_one.at[b, :, pl.ds(128 * t, 128)], out_one.at[b, :, pl.ds(at, 128)])
    for b in range(bands):
        c = jnp.transpose(tile_b[b])
        for k, first, size in segments(n):
            add(k, b, c[first:first + size])
    for new, out in zip(news[1:], outs[1:]):
        send(new, out)
    for copy in copies:
        copy.wait()


def swap(values, axis, counts):
    sizes = [counts[name] for name in ("row", "col")]
    along = ("row", "col").index(axis)
    out = []
    for k, value in enumerate(values):
        moves = []
        for i in range(sizes[0] * sizes[1]):
            place = list(divmod(i, sizes[1]))
            target = list(place)
            here = place[along]
            if here % len(values) == k and here + 1 < sizes[along]:
                target[along] += 1
            elif (here - 1) % len(values) == k and here > 0:
                target[along] -= 1
            elif (place[1 - along] ^ 1) < sizes[1 - along]:
                target[1 - along] ^= 1
            else:
                continue
            moves.append((i, target[0] * sizes[1] + target[1]))
        out.append(lax.ppermute(value, ("row", "col"), moves))
    return out


def solution(mesh):
    counts = (mesh.shape["row"], mesh.shape["col"])

    def local(relief):
        shape = bands, n, m = relief.shape
        levels = [jax.ShapeDtypeStruct((bands, n >> k, m >> k), F32) for k in range(1, LEVELS + 1)]
        width = 128 * slots(bands, m)[1]
        row_part = jax.ShapeDtypeStruct((8, width), F32)
        col_part = jax.ShapeDtypeStruct((16, 128), F32)
        rim = jax.ShapeDtypeStruct((bands, 128, 128), F32)
        tall = [
            jax.ShapeDtypeStruct((bands, (lanes_of(m >> k) if k else m) // 128, PAD + (n >> k) + TAIL, 128), F32)
            for k in range(LEVELS)
        ]
        send_e, send_o, field, *mats = pl.pallas_call(
            functools.partial(edge_kernel, shape, counts),
            out_shape=[
                row_part, row_part, tall[0],
                jax.ShapeDtypeStruct((4, 256, 256), BF16),
                jax.ShapeDtypeStruct((128, 256), BF16),
                jax.ShapeDtypeStruct((m >> 2, m >> 3), BF16),
            ],
            in_specs=[pl.BlockSpec(memory_space=pltpu.HBM)],
            out_specs=[VMEM] * 6,
            scratch_shapes=[
                pltpu.VMEM((bands, HEAD + FOOT, m), F32),
                pltpu.VMEM((m // 128, bands * 64, 128), F32),
            ] + [
                pltpu.VMEM((lanes_of(m >> k) // 128, bands * 40, 128), F32) for k in range(1, LEVELS)
            ] + [
                pltpu.VMEM((8, width), F32),
                pltpu.VMEM((8, width), F32),
                pltpu.SemaphoreType.DMA((2,)),
                pltpu.SemaphoreType.DMA((m // 128,)),
            ],
            compiler_params=pltpu.CompilerParams(vmem_limit_bytes=LIMIT),
            name="edge",
        )(pltpu.with_memory_space_constraint(relief, pltpu.HBM))
        *own, rim_a, rim_b = pl.pallas_call(
            functools.partial(pyramid_kernel, shape, counts),
            out_shape=levels + [rim, rim],
            in_specs=[VMEM] * 4,
            out_specs=[VMEM] * 6,
            scratch_shapes=[pltpu.VMEM(t.shape, F32) for t in tall[1:]],
            compiler_params=pltpu.CompilerParams(vmem_limit_bytes=LIMIT),
            cost_estimate=pl.CostEstimate(flops=8_000_000_000, bytes_accessed=0, transcendentals=0),
            name="pyramid",
        )(field, *mats)
        row_e, row_o = swap((send_e, send_o), "row", mesh.shape)
        sends = pl.pallas_call(
            functools.partial(rim_kernel, shape, counts),
            out_shape=[col_part] * 3,
            in_specs=[VMEM] * 4,
            out_specs=[VMEM] * 3,
            scratch_shapes=[pltpu.VMEM((bands, 128, 128), F32)] * 2,
            compiler_params=pltpu.CompilerParams(vmem_limit_bytes=4 << 20),
            name="rim",
        )(rim_a, rim_b, row_e, row_o)
        cols = swap(sends, "col", mesh.shape)
        ends = jax.ShapeDtypeStruct((bands, n >> 1, 256), F32)
        hbm = pl.BlockSpec(memory_space=pltpu.HBM)
        out, *done = pl.pallas_call(
            functools.partial(settle_kernel, shape),
            out_shape=[levels[0], ends] + levels[1:],
            in_specs=[VMEM] * 6,
            out_specs=[hbm] + [VMEM] * 4,
            scratch_shapes=[
                pltpu.VMEM((bands, n >> 1, (m >> 1) - 256), F32), pltpu.SemaphoreType.DMA((bands,)),
            ],
            compiler_params=pltpu.CompilerParams(vmem_limit_bytes=8 << 20),
            cost_estimate=pl.CostEstimate(flops=2_000_000_000, bytes_accessed=0, transcendentals=0),
            name="settle",
        )(*own, row_e, row_o)
        return tuple(pl.pallas_call(
            functools.partial(finish_kernel, shape),
            out_shape=levels,
            in_specs=[hbm] + [VMEM] * 7,
            out_specs=[hbm] * 4,
            scratch_shapes=[pltpu.VMEM((bands, 128, 128), F32)] * 2 + [
                pltpu.VMEM(level.shape, F32) for level in [ends] + levels[1:]
            ] + [pltpu.SemaphoreType.DMA((2 * bands + LEVELS - 1,))],
            input_output_aliases={0: 0},
            compiler_params=pltpu.CompilerParams(vmem_limit_bytes=8 << 20),
            name="finish",
        )(out, *done, *cols))

    placed = P(None, "row", "col")
    return jax.shard_map(
        local, mesh=mesh, in_specs=(placed,), out_specs=(placed,) * LEVELS, check_vma=False
    )
```

```python
import functools

import jax
import jax.numpy as jnp
from jax import lax
from jax.experimental import pallas as pl
from jax.experimental.pallas import tpu as pltpu
from jax.sharding import PartitionSpec as P


F32 = jnp.float32
BF16 = jnp.bfloat16
FAR = 1 << 20
LEVELS = 4
LIMIT = 24_000_000
VMEM = pl.BlockSpec(memory_space=pltpu.VMEM)
PAD = 8
TAIL = 24


def lanes_of(cols):
    return (cols + 3 + 127) // 128 * 128


def iota(shape, dim):
    return lax.broadcasted_iota(jnp.int32, shape, dim)


def band(source, target):
    far = jnp.abs(source - 2 * target)
    return jnp.where(far == 0, 6 / 256, jnp.where(far == 1, 4 / 256, jnp.where(far == 2, 1 / 256, 0.0))).astype(F32)


def fill_blocks(mats, first, last):
    source, lane = iota((256, 256), 0), iota((256, 256), 1)
    target = jnp.where(lane <= 128, lane, jnp.where(lane == 255, -1, FAR))
    value = band(source, target)
    inside = value.astype(BF16)
    for i in range(4):
        mats[i] = inside
    source, target = iota((16, 128), 0), iota((16, 128), 1)
    mirror = jnp.where(source >= 1, band(-source, target), 0.0)
    start = (value[:16, :128] + first * mirror).astype(BF16)
    source = source + 240
    mirror = jnp.where(source == 254, band(source + 2, target), 0.0)
    end = (value[240:, :128] + last * mirror).astype(BF16)
    for i in (1, 3):
        mats[i, :16, :128] = start
    for i in (2, 3):
        mats[i, 240:, :128] = end


def rim_matrix(first, last):
    source, lane = iota((128, 256), 0), iota((128, 256), 1)
    after = source < 64
    col = jnp.where(after, 512 + source, source - 128)
    own = jnp.where(lane < 2, 256 + lane, jnp.where(lane == 127, -1, FAR))
    other = jnp.where(lane == 128, 0, jnp.where(lane == 255, 255, FAR))
    value = band(col, jnp.where(lane < 128, own, other))
    keep = jnp.where(after, 1.0 - last, 1.0 - first)
    return (value * keep).astype(BF16)


def last_matrix(cols, first, last):
    source, lane = iota((2 * cols, cols), 0), iota((2 * cols, cols), 1)
    half = cols // 2
    col = jnp.where(source < cols + cols // 2, source, source - 2 * cols)
    target = jnp.where(lane < half + 2, lane, jnp.where(lane == cols - 1, -1, FAR))
    value = band(col, target)
    value += first * jnp.where((source >= 1) & (source < cols), band(-source, target), 0.0)
    value += last * jnp.where(source == cols - 2, band(source + 2, target), 0.0)
    keep = jnp.where(col < 0, 1.0 - first, jnp.where(col >= cols, 1.0 - last, 1.0))
    return (value * keep).astype(BF16)


def split_dot(value, matrix):
    high = value.astype(BF16)
    low = (value - high.astype(F32)).astype(BF16)
    size = value.shape[0]
    if size > 80:
        return jnp.dot(
            jnp.concatenate([high, low], 1), jnp.concatenate([matrix, matrix], 0),
            preferred_element_type=F32,
        )
    both = jnp.dot(jnp.concatenate([high, low], 0), matrix, preferred_element_type=F32)
    return both[:size] + both[size:]


def columns(tiles, cols, matrices):
    blocks = cols // 256
    rim = len(tiles) > 2 * blocks
    parts = []
    for t in range(blocks):
        index = (1 if t == 0 else 0) + (2 if t == blocks - 1 else 0)
        value = jnp.concatenate(tiles[2 * t:2 * t + 2], 1)
        parts.append(split_dot(value, matrices[index][...]))
    near = iota((tiles[0].shape[0], 128), 1) < 64
    edges = [p[:, 128:] for p in parts]
    if rim:
        around = split_dot(tiles[-1], matrices[4][...])
        edges.append(around[:, 128:])
    else:
        edges.append(jnp.zeros_like(edges[0]))
    out = [
        parts[t][:, :128] + jnp.where(near, edges[t - 1], edges[t + 1])
        for t in range(blocks)
    ]
    outer = jnp.where(near, edges[blocks - 1], edges[0])
    if rim:
        outer = outer + around[:, :128]
    return out + [outer]


def rows(ref, extent):
    half = extent // 2

    def reduced(start, size):
        e = [ref[pl.ds(start + t, size, stride=2), :] for t in range(5)]
        return (e[0] + e[4]) + 4.0 * (e[1] + e[3]) + 6.0 * e[2]

    main = reduced(PAD - 2, half)
    below = reduced(PAD - 2 + extent, 8)
    above = 4.0 * ref[PAD - 1:PAD, :] + ref[PAD:PAD + 1, :]
    return jnp.concatenate([main, jnp.where(iota(below.shape, 0) == 7, above, below)], 0)


def close(ref, extent, first, last):
    @pl.when(first)
    def _():
        ref[:, PAD - 2:PAD - 1, :] = ref[:, PAD + 2:PAD + 3, :]
        ref[:, PAD - 1:PAD, :] = ref[:, PAD + 1:PAD + 2, :]

    @pl.when(last)
    def _():
        ref[:, PAD + extent:PAD + extent + 1, :] = ref[:, PAD + extent - 2:PAD + extent - 1, :]


def slots(bands, m):
    place, tiles = {}, 0
    for k in range(2, LEVELS + 1):
        for t in range(lanes_of(m >> k) // 128):
            for b in range(bands):
                place[k, t, b] = tiles, 2 * b
            tiles += 1
    free = [(j, r) for j in range(tiles) for r in range(2 * bands, 8)]
    for t in range(lanes_of(m >> 1) // 128):
        for b in range(bands):
            if not free:
                free = [(tiles, r) for r in range(8)]
                tiles += 1
            place[1, t, b] = free.pop(0)
    return place, tiles


HEAD, FOOT = 16, 32


def edge_kernel(
    shape, counts, x_hbm, send_e, send_o, s0, mats, rim_mat, end_mat,
    e1, e2, e3, down, up, sems,
):
    bands, n, m = shape
    row, col = lax.axis_index("row"), lax.axis_index("col")
    top, bottom = row == 0, row == counts[0] - 1

    def load(start, size, t, sem):
        return pltpu.make_async_copy(
            x_hbm.at[:, pl.ds(start, size), pl.ds(128 * t, 128)],
            s0.at[:, t, pl.ds(PAD + start, size), :], sem,
        )

    def wait(size, sem):
        whole = x_hbm.at[:, pl.ds(0, size), :]
        pltpu.make_async_copy(whole, whole, sem).wait()

    for t in range(m // 128):
        load(0, HEAD, t, sems.at[0]).start()
        load(n - FOOT, FOOT, t, sems.at[0]).start()
    for t in range(m // 128):
        load(HEAD, n - HEAD - FOOT, t, sems.at[1]).start()
    left = jnp.where(col == 0, 1.0, 0.0).astype(F32)
    right = jnp.where(col == counts[1] - 1, 1.0, 0.0).astype(F32)
    fill_blocks(mats, left, right)
    rim_mat[...] = rim_matrix(left, right)
    end_mat[...] = last_matrix(end_mat.shape[1], left, right)
    matrices = [mats.at[i] for i in range(4)] + [rim_mat]
    s0[:, :, 0:PAD, :] = jnp.zeros(s0.shape[:2] + (PAD, 128), F32)
    s0[:, :, PAD + n:, :] = jnp.zeros(s0.shape[:2] + (TAIL, 128), F32)
    down[...] = jnp.zeros_like(down)
    up[...] = jnp.zeros_like(up)
    for ref, filled in zip((e1, e2, e3), (24, 16, 16)):
        for b in range(bands):
            ref[:, 40 * b:40 * b + 8, :] = jnp.zeros((ref.shape[0], 8, 128), F32)
            rest = 32 - filled
            ref[:, 40 * (b + 1) - rest:40 * (b + 1), :] = jnp.zeros((ref.shape[0], rest, 128), F32)
    wait(HEAD + FOOT, sems.at[0])
    place, _ = slots(bands, m)
    for k, ref in enumerate((s0, e1, e2, e3)):
        head, foot, size = ((PAD - 4, PAD + n - FOOT, 16), (5, 17, 8), (5, 16, 8), (5, 16, 8))[k]

        def reduced(b, t, start, size):
            lines = [pl.ds(start + i + (40 * b if k else 0), size, stride=2) for i in range(5)]
            e = [ref[t, line, :] if k else ref[b, t, line, :] for line in lines]
            return (e[0] + e[4]) + 4.0 * (e[1] + e[3]) + 6.0 * e[2]

        tiles = [
            jnp.concatenate(
                [
                    part for b in range(bands) for part in (
                        reduced(b, t, head, 8), reduced(b, t, foot, size)
                    )
                ],
                0,
            )
            for t in range(ref.shape[0] if k else m // 128)
        ]
        if k < LEVELS - 1:
            tiles = columns(tiles, m >> k, matrices)
        else:
            tiles = [split_dot(jnp.concatenate(tiles, 1), end_mat[...])]
        held = 8 + size
        first, count = ((23, 1), (14, 2), (10, 2), (8, 2))[k]
        for t, tile in enumerate(tiles):
            for b in range(bands):
                if k < LEVELS - 1:
                    (e1, e2, e3)[k][t, 40 * b + 8:40 * b + 8 + held, :] = tile[held * b:held * b + held]
                spot, line = place[k + 1, t, b]
                wide = pl.ds(128 * spot, 128)
                down[line:line + count, wide] = tile[held * b + first:held * b + first + count]
                up[line:line + 1, wide] = tile[held * b:held * b + 1]
    lower_part = jnp.where(bottom, 0.0, down[...])
    upper_part = jnp.where(top, 0.0, up[...])
    even = (row & 1) == 0
    send_e[...] = jnp.where(even, lower_part, upper_part)
    send_o[...] = jnp.where(even, upper_part, lower_part)
    wait(n - HEAD - FOOT, sems.at[1])
    for b in range(bands):
        close(s0.at[b], n, top, bottom)


def pyramid_kernel(
    shape, counts, s0, mats, rim_mat, end_mat, one, two, three, four, rim_a, rim_b, s1, s2, s3,
):
    bands, n, m = shape
    row = lax.axis_index("row")
    top, bottom = row == 0, row == counts[0] - 1
    matrices = [mats.at[i] for i in range(4)] + [rim_mat]
    fields, outs = [s0, s1, s2, s3], [one, two, three, four]
    sub = iota((8, 128), 0)

    def store(k, b, t, tile):
        half = n >> (k + 1)
        tail, after = tile[half:], fields[k + 1]
        after[b, t, PAD:PAD + half, :] = tile[:half]
        after[b, t, 0:PAD, :] = jnp.where(sub == 7, tail, 0.0)
        after[b, t, PAD + half:PAD + half + 8, :] = jnp.where(sub < 2, tail, 0.0)
        after[b, t, PAD + half + 8:, :] = jnp.zeros((TAIL - 8, 128), F32)
        if 128 * t < outs[k].shape[2]:
            outs[k][b, :, 128 * t:128 * t + 128] = tile[:half]
        elif k == 0:
            rim_a[b] = tile[:half]

    def level_one(b, _):
        tiles = columns([rows(s0.at[b, t], n) for t in range(m // 128)], m, matrices)
        for t, tile in enumerate(tiles):
            store(0, b, t, tile)
        return 0

    lax.fori_loop(0, bands, level_one, 0)
    start = 0
    for k in range(1, LEVELS):
        extent, cols = n >> k, m >> k
        half = extent // 2
        for b in range(bands):
            close(fields[k].at[b], extent, top, bottom)
        tiles = [
            jnp.concatenate([rows(fields[k].at[b, t], extent) for b in range(bands)], 0)
            for t in range(fields[k].shape[1])
        ]
        if k < LEVELS - 1:
            tiles = columns(tiles, cols, matrices)
        else:
            tiles = [split_dot(jnp.concatenate(tiles, 1), end_mat[...])]
        for b in range(bands):
            parts = [tile[(half + 8) * b:(half + 8) * (b + 1)] for tile in tiles]
            body = parts[-1][:half]
            if k < LEVELS - 1:
                for t, tile in enumerate(parts):
                    store(k, b, t, tile)
            else:
                four[b] = body[:, :cols // 2]
                body = jnp.where(iota(body.shape, 1) < 2, pltpu.roll(body, 128 - cols // 2, 1), body)
            rim_b[b, start:start + half, :] = body
        start += half
    rim_b[:, start:, :] = jnp.zeros((bands, 128 - start, 128), F32)


def from_rows(got_e, got_o):
    even = (lax.axis_index("row") & 1) == 0
    e, o = got_e[...], got_o[...]
    return jnp.where(even, o, e), jnp.where(even, e, o)


def row_parts(above, below, place, k, t, b):
    spot, line = place[k, t, b]
    head, foot = (part[:, 128 * spot:128 * spot + 128] for part in (above, below))
    sub = iota(head.shape, 0)
    head = pltpu.roll(head, 8 - line, 0) if line else head
    foot = pltpu.roll(foot, 7 - line, 0) if line < 7 else foot
    return jnp.where(sub < (1 if k == 1 else 2), head, 0.0), jnp.where(sub == 7, foot, 0.0)


def segments(n):
    out, start = [], 0
    for k in range(2, LEVELS + 1):
        out.append((k, start, n >> k))
        start += n >> k
    return out


def rim_kernel(
    shape, counts, rim_a, rim_b, got_e, got_o, send_0, send_1, send_2, tile_a, tile_b
):
    bands, n, m = shape
    above, below = from_rows(got_e, got_o)
    place, _ = slots(bands, m)

    def rim_of(k, b):
        parts = row_parts(above, below, place, k, (m >> k) // 128, b)
        if (m >> k) < 128:
            parts = [jnp.where(iota(p.shape, 1) < 2, pltpu.roll(p, 128 - (m >> k), 1), p) for p in parts]
        return parts

    sub = iota((16, 128), 0)
    to_right, to_left = jnp.zeros((16, 128), F32), jnp.zeros((16, 128), F32)
    for b in range(bands):
        half = n // 2
        tile_a[b] = rim_a[b]
        tile_b[b] = rim_b[b]
        for ref, k, first, size in [(tile_a, 1, 0, half)] + [(tile_b, k, s, z) for k, s, z in segments(n)]:
            head, foot = rim_of(k, b)
            ref[b, first:first + 8, :] += head
            ref[b, first + size - 8:first + size, :] += foot
        a = jnp.transpose(tile_a[b])
        c = jnp.transpose(tile_b[b])
        to_right = jnp.where(sub == 4 * b, a[0:1], to_right)
        to_right = jnp.where(sub == 4 * b + 1, c[0:1], to_right)
        to_right = jnp.where(sub == 4 * b + 2, c[1:2], to_right)
        to_left = jnp.where(sub == 4 * b, a[127:128], to_left)
        to_left = jnp.where(sub == 4 * b + 1, c[127:128], to_left)
    col = lax.axis_index("col")
    to_right = jnp.where(col == counts[1] - 1, 0.0, to_right)
    to_left = jnp.where(col == 0, 0.0, to_left)
    for k, send in enumerate((send_0, send_1, send_2)):
        left = jnp.where((col + 2) % 3 == k, to_left, 0.0)
        send[...] = jnp.where(col % 3 == k, to_right, left)


def settle_kernel(
    shape, one, two, three, four, row_e, row_o, out, done_one, done_two, done_three, done_four, inner, sems
):
    bands, n, m = shape
    above, below = from_rows(row_e, row_o)
    place, _ = slots(bands, m)
    tiles = (m >> 1) // 128
    copies = []
    for b in range(bands):
        for k, (field, done) in enumerate(zip((one, two, three, four), (done_one, done_two, done_three, done_four)), 1):
            cols, size = m >> k, n >> k
            wide = min(cols, 128)
            for t in range(cols // wide):
                at, to, ref = pl.ds(wide * t, wide), pl.ds(wide * t, wide), done
                if k == 1:
                    if 0 < t < tiles - 1:
                        ref, to = inner, pl.ds(128 * (t - 1), 128)
                    else:
                        to = pl.ds(128 * min(t, 1), 128)
                head, foot = row_parts(above, below, place, k, t, b)
                ref[b, 0:8, to] = field[b, 0:8, at] + head[:, :wide]
                if size > 16:
                    ref[b, 8:size - 8, to] = field[b, 8:size - 8, at]
                ref[b, size - 8:size, to] = field[b, size - 8:size, at] + foot[:, :wide]
            if k == 1:
                copy = pltpu.make_async_copy(
                    inner.at[b], out.at[b, :, pl.ds(128, 128 * (tiles - 2))], sems.at[b]
                )
                copy.start()
                copies.append(copy)
    for copy in copies:
        copy.wait()


def finish_kernel(
    shape, _, one, two, three, four, col_0, col_1, col_2,
    out_one, out_two, out_three, out_four, tile_a, tile_b, new_one, new_two, new_three, new_four, sems,
):
    bands, n, m = shape
    turn = lax.axis_index("col") % 3
    got = [col_0[...], col_1[...], col_2[...]]
    after = jnp.where(turn == 0, got[0], jnp.where(turn == 1, got[1], got[2]))
    before = jnp.where(turn == 0, got[2], jnp.where(turn == 1, got[0], got[1]))
    fields, news = [one, two, three, four], [new_one, new_two, new_three, new_four]
    outs = [out_one, out_two, out_three, out_four]
    tile_a[...] = jnp.zeros_like(tile_a)
    tile_b[...] = jnp.zeros_like(tile_b)
    lane = iota((128, 128), 1)
    copies = []

    def send(source, target):
        copy = pltpu.make_async_copy(source, target, sems.at[len(copies)])
        copy.start()
        copies.append(copy)

    def add(k, b, part):
        cols, size = m >> k, part.shape[0]
        wide = min(cols, 128)
        spot = lane[:size, :wide]
        part = part[:, :wide]
        low, high = jnp.where(spot < 2, part, 0.0), jnp.where(spot == wide - 1, part, 0.0)
        count = min(cols // wide, 2)
        for t in range(count):
            at = pl.ds(wide * t, wide)
            value = fields[k - 1][b, :, at]
            if t == 0:
                value = value + low
            if t == count - 1:
                value = value + high
            news[k - 1][b, :, at] = value

    for b in range(bands):
        tile_a[b, 0:1, :] = before[4 * b:4 * b + 1]
        tile_a[b, 127:128, :] = after[4 * b:4 * b + 1]
        tile_b[b, 0:2, :] = before[4 * b + 1:4 * b + 3]
        tile_b[b, 127:128, :] = after[4 * b + 1:4 * b + 2]
        tile_b[b, 63:64, :] = after[4 * b + 1:4 * b + 2]
    for b in range(bands):
        add(1, b, jnp.transpose(tile_a[b]))
        for t, at in enumerate((0, (m >> 1) - 128)):
            send(new_one.at[b, :, pl.ds(128 * t, 128)], out_one.at[b, :, pl.ds(at, 128)])
    for b in range(bands):
        c = jnp.transpose(tile_b[b])
        for k, first, size in segments(n):
            add(k, b, c[first:first + size])
    for new, out in zip(news[1:], outs[1:]):
        send(new, out)
    for copy in copies:
        copy.wait()


def swap(values, axis, counts):
    sizes = [counts[name] for name in ("row", "col")]
    along = ("row", "col").index(axis)
    out = []
    for k, value in enumerate(values):
        moves = []
        for i in range(sizes[0] * sizes[1]):
            place = list(divmod(i, sizes[1]))
            target = list(place)
            here = place[along]
            if here % len(values) == k and here + 1 < sizes[along]:
                target[along] += 1
            elif (here - 1) % len(values) == k and here > 0:
                target[along] -= 1
            elif (place[1 - along] ^ 1) < sizes[1 - along]:
                target[1 - along] ^= 1
            else:
                continue
            moves.append((i, target[0] * sizes[1] + target[1]))
        out.append(lax.ppermute(value, ("row", "col"), moves))
    return out


def solution(mesh):
    counts = (mesh.shape["row"], mesh.shape["col"])

    def local(relief):
        shape = bands, n, m = relief.shape
        levels = [jax.ShapeDtypeStruct((bands, n >> k, m >> k), F32) for k in range(1, LEVELS + 1)]
        width = 128 * slots(bands, m)[1]
        row_part = jax.ShapeDtypeStruct((8, width), F32)
        col_part = jax.ShapeDtypeStruct((16, 128), F32)
        rim = jax.ShapeDtypeStruct((bands, 128, 128), F32)
        tall = [
            jax.ShapeDtypeStruct((bands, (lanes_of(m >> k) if k else m) // 128, PAD + (n >> k) + TAIL, 128), F32)
            for k in range(LEVELS)
        ]
        send_e, send_o, field, *mats = pl.pallas_call(
            functools.partial(edge_kernel, shape, counts),
            out_shape=[
                row_part, row_part, tall[0],
                jax.ShapeDtypeStruct((4, 256, 256), BF16),
                jax.ShapeDtypeStruct((128, 256), BF16),
                jax.ShapeDtypeStruct((m >> 2, m >> 3), BF16),
            ],
            in_specs=[pl.BlockSpec(memory_space=pltpu.HBM)],
            out_specs=[VMEM] * 6,
            scratch_shapes=[
                pltpu.VMEM((lanes_of(m >> k) // 128, bands * 40, 128), F32) for k in range(1, LEVELS)
            ] + [
                pltpu.VMEM((8, width), F32),
                pltpu.VMEM((8, width), F32),
                pltpu.SemaphoreType.DMA((2,)),
            ],
            compiler_params=pltpu.CompilerParams(vmem_limit_bytes=LIMIT),
            name="edge",
        )(pltpu.with_memory_space_constraint(relief, pltpu.HBM))
        *own, rim_a, rim_b = pl.pallas_call(
            functools.partial(pyramid_kernel, shape, counts),
            out_shape=levels + [rim, rim],
            in_specs=[VMEM] * 4,
            out_specs=[VMEM] * 6,
            scratch_shapes=[pltpu.VMEM(t.shape, F32) for t in tall[1:]],
            compiler_params=pltpu.CompilerParams(vmem_limit_bytes=LIMIT),
            cost_estimate=pl.CostEstimate(flops=8_000_000_000, bytes_accessed=0, transcendentals=0),
            name="pyramid",
        )(field, *mats)
        row_e, row_o = swap((send_e, send_o), "row", mesh.shape)
        sends = pl.pallas_call(
            functools.partial(rim_kernel, shape, counts),
            out_shape=[col_part] * 3,
            in_specs=[VMEM] * 4,
            out_specs=[VMEM] * 3,
            scratch_shapes=[pltpu.VMEM((bands, 128, 128), F32)] * 2,
            compiler_params=pltpu.CompilerParams(vmem_limit_bytes=4 << 20),
            name="rim",
        )(rim_a, rim_b, row_e, row_o)
        cols = swap(sends, "col", mesh.shape)
        ends = jax.ShapeDtypeStruct((bands, n >> 1, 256), F32)
        hbm = pl.BlockSpec(memory_space=pltpu.HBM)
        out, *done = pl.pallas_call(
            functools.partial(settle_kernel, shape),
            out_shape=[levels[0], ends] + levels[1:],
            in_specs=[VMEM] * 6,
            out_specs=[hbm] + [VMEM] * 4,
            scratch_shapes=[
                pltpu.VMEM((bands, n >> 1, (m >> 1) - 256), F32), pltpu.SemaphoreType.DMA((bands,)),
            ],
            compiler_params=pltpu.CompilerParams(vmem_limit_bytes=8 << 20),
            cost_estimate=pl.CostEstimate(flops=2_000_000_000, bytes_accessed=0, transcendentals=0),
            name="settle",
        )(*own, row_e, row_o)
        return tuple(pl.pallas_call(
            functools.partial(finish_kernel, shape),
            out_shape=levels,
            in_specs=[hbm] + [VMEM] * 7,
            out_specs=[hbm] * 4,
            scratch_shapes=[pltpu.VMEM((bands, 128, 128), F32)] * 2 + [
                pltpu.VMEM(level.shape, F32) for level in [ends] + levels[1:]
            ] + [pltpu.SemaphoreType.DMA((2 * bands + LEVELS - 1,))],
            input_output_aliases={0: 0},
            compiler_params=pltpu.CompilerParams(vmem_limit_bytes=8 << 20),
            name="finish",
        )(out, *done, *cols))

    placed = P(None, "row", "col")
    return jax.shard_map(
        local, mesh=mesh, in_specs=(placed,), out_specs=(placed,) * LEVELS, check_vma=False
    )
```

```python
import functools

import jax
import jax.numpy as jnp
from jax import lax
from jax.experimental import pallas as pl
from jax.experimental.pallas import tpu as pltpu
from jax.sharding import PartitionSpec as P


F32 = jnp.float32
BF16 = jnp.bfloat16
FAR = 1 << 20
LEVELS = 4
LIMIT = 24_000_000
VMEM = pl.BlockSpec(memory_space=pltpu.VMEM)
PAD = 8
TAIL = 24


def lanes_of(cols):
    return (cols + 3 + 127) // 128 * 128


def iota(shape, dim):
    return lax.broadcasted_iota(jnp.int32, shape, dim)


def band(source, target):
    far = jnp.abs(source - 2 * target)
    return jnp.where(far == 0, 6 / 256, jnp.where(far == 1, 4 / 256, jnp.where(far == 2, 1 / 256, 0.0))).astype(F32)


def fill_blocks(mats, first, last):
    source, lane = iota((256, 256), 0), iota((256, 256), 1)
    target = jnp.where(lane <= 128, lane, jnp.where(lane == 255, -1, FAR))
    value = band(source, target)
    inside = value.astype(BF16)
    for i in range(4):
        mats[i] = inside
    source, target = iota((16, 128), 0), iota((16, 128), 1)
    mirror = jnp.where(source >= 1, band(-source, target), 0.0)
    start = (value[:16, :128] + first * mirror).astype(BF16)
    source = source + 240
    mirror = jnp.where(source == 254, band(source + 2, target), 0.0)
    end = (value[240:, :128] + last * mirror).astype(BF16)
    for i in (1, 3):
        mats[i, :16, :128] = start
    for i in (2, 3):
        mats[i, 240:, :128] = end


def rim_matrix(first, last):
    source, lane = iota((128, 256), 0), iota((128, 256), 1)
    after = source < 64
    col = jnp.where(after, 512 + source, source - 128)
    own = jnp.where(lane < 2, 256 + lane, jnp.where(lane == 127, -1, FAR))
    other = jnp.where(lane == 128, 0, jnp.where(lane == 255, 255, FAR))
    value = band(col, jnp.where(lane < 128, own, other))
    keep = jnp.where(after, 1.0 - last, 1.0 - first)
    return (value * keep).astype(BF16)


def last_matrix(cols, first, last):
    source, lane = iota((2 * cols, cols), 0), iota((2 * cols, cols), 1)
    half = cols // 2
    col = jnp.where(source < cols + cols // 2, source, source - 2 * cols)
    target = jnp.where(lane < half + 2, lane, jnp.where(lane == cols - 1, -1, FAR))
    value = band(col, target)
    value += first * jnp.where((source >= 1) & (source < cols), band(-source, target), 0.0)
    value += last * jnp.where(source == cols - 2, band(source + 2, target), 0.0)
    keep = jnp.where(col < 0, 1.0 - first, jnp.where(col >= cols, 1.0 - last, 1.0))
    return (value * keep).astype(BF16)


def split_dot(value, matrix):
    high = value.astype(BF16)
    low = (value - high.astype(F32)).astype(BF16)
    size = value.shape[0]
    if size > 80:
        return jnp.dot(
            jnp.concatenate([high, low], 1), jnp.concatenate([matrix, matrix], 0),
            preferred_element_type=F32,
        )
    both = jnp.dot(jnp.concatenate([high, low], 0), matrix, preferred_element_type=F32)
    return both[:size] + both[size:]


def columns(tiles, cols, matrices):
    blocks = cols // 256
    rim = len(tiles) > 2 * blocks
    parts = []
    for t in range(blocks):
        index = (1 if t == 0 else 0) + (2 if t == blocks - 1 else 0)
        value = jnp.concatenate(tiles[2 * t:2 * t + 2], 1)
        parts.append(split_dot(value, matrices[index][...]))
    near = iota((tiles[0].shape[0], 128), 1) < 64
    edges = [p[:, 128:] for p in parts]
    if rim:
        around = split_dot(tiles[-1], matrices[4][...])
        edges.append(around[:, 128:])
    else:
        edges.append(jnp.zeros_like(edges[0]))
    out = [
        parts[t][:, :128] + jnp.where(near, edges[t - 1], edges[t + 1])
        for t in range(blocks)
    ]
    outer = jnp.where(near, edges[blocks - 1], edges[0])
    if rim:
        outer = outer + around[:, :128]
    return out + [outer]


def rows(ref, extent):
    half = extent // 2

    def reduced(start, size):
        e = [ref[pl.ds(start + t, size, stride=2), :] for t in range(5)]
        return (e[0] + e[4]) + 4.0 * (e[1] + e[3]) + 6.0 * e[2]

    main = reduced(PAD - 2, half)
    below = reduced(PAD - 2 + extent, 8)
    above = 4.0 * ref[PAD - 1:PAD, :] + ref[PAD:PAD + 1, :]
    return jnp.concatenate([main, jnp.where(iota(below.shape, 0) == 7, above, below)], 0)


def close(ref, extent, first, last):
    @pl.when(first)
    def _():
        ref[:, PAD - 2:PAD - 1, :] = ref[:, PAD + 2:PAD + 3, :]
        ref[:, PAD - 1:PAD, :] = ref[:, PAD + 1:PAD + 2, :]

    @pl.when(last)
    def _():
        ref[:, PAD + extent:PAD + extent + 1, :] = ref[:, PAD + extent - 2:PAD + extent - 1, :]


def slots(bands, m):
    place, tiles = {}, 0
    for k in range(2, LEVELS + 1):
        for t in range(lanes_of(m >> k) // 128):
            for b in range(bands):
                place[k, t, b] = tiles, 2 * b
            tiles += 1
    free = [(j, r) for j in range(tiles) for r in range(2 * bands, 8)]
    for t in range(lanes_of(m >> 1) // 128):
        for b in range(bands):
            if not free:
                free = [(tiles, r) for r in range(8)]
                tiles += 1
            place[1, t, b] = free.pop(0)
    return place, tiles


HEAD, FOOT = 16, 32


def edge_kernel(
    shape, counts, x_hbm, send_e, send_o, s0, mats, rim_mat, end_mat,
    e1, e2, e3, down, up, sems,
):
    bands, n, m = shape
    row, col = lax.axis_index("row"), lax.axis_index("col")
    top, bottom = row == 0, row == counts[0] - 1

    def load(start, size, t, sem):
        return pltpu.make_async_copy(
            x_hbm.at[:, pl.ds(start, size), pl.ds(128 * t, 128)],
            s0.at[:, t, pl.ds(PAD + start, size), :], sem,
        )

    def wait(size, sem):
        whole = x_hbm.at[:, pl.ds(0, size), :]
        pltpu.make_async_copy(whole, whole, sem).wait()

    for t in range(m // 128):
        load(0, HEAD, t, sems.at[0]).start()
        load(n - FOOT, FOOT, t, sems.at[0]).start()
    part = (n - HEAD - FOOT) // 2
    for i in range(2):
        for t in range(m // 128):
            load(HEAD + part * i, part, t, sems.at[1]).start()
    left = jnp.where(col == 0, 1.0, 0.0).astype(F32)
    right = jnp.where(col == counts[1] - 1, 1.0, 0.0).astype(F32)
    fill_blocks(mats, left, right)
    rim_mat[...] = rim_matrix(left, right)
    end_mat[...] = last_matrix(end_mat.shape[1], left, right)
    matrices = [mats.at[i] for i in range(4)] + [rim_mat]
    s0[:, :, 0:PAD, :] = jnp.zeros(s0.shape[:2] + (PAD, 128), F32)
    s0[:, :, PAD + n:, :] = jnp.zeros(s0.shape[:2] + (TAIL, 128), F32)
    down[...] = jnp.zeros_like(down)
    up[...] = jnp.zeros_like(up)
    for ref, filled in zip((e1, e2, e3), (24, 16, 16)):
        for b in range(bands):
            ref[:, 40 * b:40 * b + 8, :] = jnp.zeros((ref.shape[0], 8, 128), F32)
            rest = 32 - filled
            ref[:, 40 * (b + 1) - rest:40 * (b + 1), :] = jnp.zeros((ref.shape[0], rest, 128), F32)
    wait(HEAD + FOOT, sems.at[0])
    place, _ = slots(bands, m)
    for k, ref in enumerate((s0, e1, e2, e3)):
        head, foot, size = ((PAD - 4, PAD + n - FOOT, 16), (5, 17, 8), (5, 16, 8), (5, 16, 8))[k]

        def reduced(b, t, start, size):
            lines = [pl.ds(start + i + (40 * b if k else 0), size, stride=2) for i in range(5)]
            e = [ref[t, line, :] if k else ref[b, t, line, :] for line in lines]
            return (e[0] + e[4]) + 4.0 * (e[1] + e[3]) + 6.0 * e[2]

        tiles = [
            jnp.concatenate(
                [
                    part for b in range(bands) for part in (
                        reduced(b, t, head, 8), reduced(b, t, foot, size)
                    )
                ],
                0,
            )
            for t in range(ref.shape[0] if k else m // 128)
        ]
        if k < LEVELS - 1:
            tiles = columns(tiles, m >> k, matrices)
        else:
            tiles = [split_dot(jnp.concatenate(tiles, 1), end_mat[...])]
        held = 8 + size
        first, count = ((23, 1), (14, 2), (10, 2), (8, 2))[k]
        for t, tile in enumerate(tiles):
            for b in range(bands):
                if k < LEVELS - 1:
                    (e1, e2, e3)[k][t, 40 * b + 8:40 * b + 8 + held, :] = tile[held * b:held * b + held]
                spot, line = place[k + 1, t, b]
                wide = pl.ds(128 * spot, 128)
                down[line:line + count, wide] = tile[held * b + first:held * b + first + count]
                up[line:line + 1, wide] = tile[held * b:held * b + 1]
    lower_part = jnp.where(bottom, 0.0, down[...])
    upper_part = jnp.where(top, 0.0, up[...])
    even = (row & 1) == 0
    send_e[...] = jnp.where(even, lower_part, upper_part)
    send_o[...] = jnp.where(even, upper_part, lower_part)
    wait(n - HEAD - FOOT, sems.at[1])
    for b in range(bands):
        close(s0.at[b], n, top, bottom)


def pyramid_kernel(
    shape, counts, s0, mats, rim_mat, end_mat, s1, s2, s3, four, rim_a, rim_b,
):
    bands, n, m = shape
    row = lax.axis_index("row")
    top, bottom = row == 0, row == counts[0] - 1
    matrices = [mats.at[i] for i in range(4)] + [rim_mat]
    fields = [s0, s1, s2, s3]
    sub = iota((8, 128), 0)

    def store(k, b, t, tile):
        half = n >> (k + 1)
        tail, after = tile[half:], fields[k + 1]
        after[b, t, PAD:PAD + half, :] = tile[:half]
        after[b, t, 0:PAD, :] = jnp.where(sub == 7, tail, 0.0)
        after[b, t, PAD + half:PAD + half + 8, :] = jnp.where(sub < 2, tail, 0.0)
        after[b, t, PAD + half + 8:, :] = jnp.zeros((TAIL - 8, 128), F32)
        if k == 0 and t == after.shape[1] - 1:
            rim_a[b] = tile[:half]

    def level_one(b, _):
        tiles = columns([rows(s0.at[b, t], n) for t in range(m // 128)], m, matrices)
        for t, tile in enumerate(tiles):
            store(0, b, t, tile)
        return 0

    lax.fori_loop(0, bands, level_one, 0)
    start = 0
    for k in range(1, LEVELS):
        extent, cols = n >> k, m >> k
        half = extent // 2
        for b in range(bands):
            close(fields[k].at[b], extent, top, bottom)
        tiles = [
            jnp.concatenate([rows(fields[k].at[b, t], extent) for b in range(bands)], 0)
            for t in range(fields[k].shape[1])
        ]
        if k < LEVELS - 1:
            tiles = columns(tiles, cols, matrices)
        else:
            tiles = [split_dot(jnp.concatenate(tiles, 1), end_mat[...])]
        for b in range(bands):
            parts = [tile[(half + 8) * b:(half + 8) * (b + 1)] for tile in tiles]
            body = parts[-1][:half]
            if k < LEVELS - 1:
                for t, tile in enumerate(parts):
                    store(k, b, t, tile)
            else:
                four[b] = body[:, :cols // 2]
                body = jnp.where(iota(body.shape, 1) < 2, pltpu.roll(body, 128 - cols // 2, 1), body)
            rim_b[b, start:start + half, :] = body
        start += half
    rim_b[:, start:, :] = jnp.zeros((bands, 128 - start, 128), F32)


def from_rows(got_e, got_o):
    even = (lax.axis_index("row") & 1) == 0
    e, o = got_e[...], got_o[...]
    return jnp.where(even, o, e), jnp.where(even, e, o)


def row_parts(above, below, place, k, t, b):
    spot, line = place[k, t, b]
    head, foot = (part[:, 128 * spot:128 * spot + 128] for part in (above, below))
    sub = iota(head.shape, 0)
    head = pltpu.roll(head, 8 - line, 0) if line else head
    foot = pltpu.roll(foot, 7 - line, 0) if line < 7 else foot
    return jnp.where(sub < (1 if k == 1 else 2), head, 0.0), jnp.where(sub == 7, foot, 0.0)


def segments(n):
    out, start = [], 0
    for k in range(2, LEVELS + 1):
        out.append((k, start, n >> k))
        start += n >> k
    return out


def rim_kernel(
    shape, counts, rim_a, rim_b, got_e, got_o, send_0, send_1, send_2, tile_a, tile_b
):
    bands, n, m = shape
    above, below = from_rows(got_e, got_o)
    place, _ = slots(bands, m)

    def rim_of(k, b):
        parts = row_parts(above, below, place, k, (m >> k) // 128, b)
        if (m >> k) < 128:
            parts = [jnp.where(iota(p.shape, 1) < 2, pltpu.roll(p, 128 - (m >> k), 1), p) for p in parts]
        return parts

    sub = iota((16, 128), 0)
    to_right, to_left = jnp.zeros((16, 128), F32), jnp.zeros((16, 128), F32)
    for b in range(bands):
        half = n // 2
        tile_a[b] = rim_a[b]
        tile_b[b] = rim_b[b]
        for ref, k, first, size in [(tile_a, 1, 0, half)] + [(tile_b, k, s, z) for k, s, z in segments(n)]:
            head, foot = rim_of(k, b)
            ref[b, first:first + 8, :] += head
            ref[b, first + size - 8:first + size, :] += foot
        a = jnp.transpose(tile_a[b])
        c = jnp.transpose(tile_b[b])
        to_right = jnp.where(sub == 4 * b, a[0:1], to_right)
        to_right = jnp.where(sub == 4 * b + 1, c[0:1], to_right)
        to_right = jnp.where(sub == 4 * b + 2, c[1:2], to_right)
        to_left = jnp.where(sub == 4 * b, a[127:128], to_left)
        to_left = jnp.where(sub == 4 * b + 1, c[127:128], to_left)
    col = lax.axis_index("col")
    to_right = jnp.where(col == counts[1] - 1, 0.0, to_right)
    to_left = jnp.where(col == 0, 0.0, to_left)
    for k, send in enumerate((send_0, send_1, send_2)):
        left = jnp.where((col + 2) % 3 == k, to_left, 0.0)
        send[...] = jnp.where(col % 3 == k, to_right, left)


def settle_kernel(
    shape, one, two, three, four, row_e, row_o, out, done_one, done_two, done_three, done_four, inner, sems
):
    bands, n, m = shape
    above, below = from_rows(row_e, row_o)
    place, _ = slots(bands, m)
    tiles = (m >> 1) // 128
    copies = []
    for b in range(bands):
        for k, (field, done) in enumerate(zip((one, two, three, four), (done_one, done_two, done_three, done_four)), 1):
            cols, size = m >> k, n >> k
            wide = min(cols, 128)
            for t in range(cols // wide):
                to, ref = pl.ds(wide * t, wide), done
                if k == 1:
                    if 0 < t < tiles - 1:
                        ref, to = inner, pl.ds(128 * (t - 1), 128)
                    else:
                        to = pl.ds(128 * min(t, 1), 128)
                head, foot = row_parts(above, below, place, k, t, b)
                own = field.at[b] if k == LEVELS else field.at[b, t, pl.ds(PAD, size), :]
                ref[b, 0:8, to] = own[0:8, :] + head[:, :wide]
                if size > 16:
                    ref[b, 8:size - 8, to] = own[8:size - 8, :]
                ref[b, size - 8:size, to] = own[size - 8:size, :] + foot[:, :wide]
            if k == 1:
                copy = pltpu.make_async_copy(
                    inner.at[b], out.at[b, :, pl.ds(128, 128 * (tiles - 2))], sems.at[b]
                )
                copy.start()
                copies.append(copy)
    for copy in copies:
        copy.wait()


def finish_kernel(
    shape, _, one, two, three, four, col_0, col_1, col_2,
    out_one, out_two, out_three, out_four, tile_a, tile_b, new_one, new_two, new_three, new_four, sems,
):
    bands, n, m = shape
    turn = lax.axis_index("col") % 3
    got = [col_0[...], col_1[...], col_2[...]]
    after = jnp.where(turn == 0, got[0], jnp.where(turn == 1, got[1], got[2]))
    before = jnp.where(turn == 0, got[2], jnp.where(turn == 1, got[0], got[1]))
    fields, news = [one, two, three, four], [new_one, new_two, new_three, new_four]
    outs = [out_one, out_two, out_three, out_four]
    tile_a[...] = jnp.zeros_like(tile_a)
    tile_b[...] = jnp.zeros_like(tile_b)
    lane = iota((128, 128), 1)
    copies = []

    def send(source, target):
        copy = pltpu.make_async_copy(source, target, sems.at[len(copies)])
        copy.start()
        copies.append(copy)

    def add(k, b, part):
        cols, size = m >> k, part.shape[0]
        wide = min(cols, 128)
        spot = lane[:size, :wide]
        part = part[:, :wide]
        low, high = jnp.where(spot < 2, part, 0.0), jnp.where(spot == wide - 1, part, 0.0)
        count = min(cols // wide, 2)
        for t in range(count):
            at = pl.ds(wide * t, wide)
            value = fields[k - 1][b, :, at]
            if t == 0:
                value = value + low
            if t == count - 1:
                value = value + high
            news[k - 1][b, :, at] = value

    for b in range(bands):
        tile_a[b, 0:1, :] = before[4 * b:4 * b + 1]
        tile_a[b, 127:128, :] = after[4 * b:4 * b + 1]
        tile_b[b, 0:2, :] = before[4 * b + 1:4 * b + 3]
        tile_b[b, 127:128, :] = after[4 * b + 1:4 * b + 2]
        tile_b[b, 63:64, :] = after[4 * b + 1:4 * b + 2]
    for b in range(bands):
        add(1, b, jnp.transpose(tile_a[b]))
        for t, at in enumerate((0, (m >> 1) - 128)):
            send(new_one.at[b, :, pl.ds(128 * t, 128)], out_one.at[b, :, pl.ds(at, 128)])
    for b in range(bands):
        c = jnp.transpose(tile_b[b])
        for k, first, size in segments(n):
            add(k, b, c[first:first + size])
    for new, out in zip(news[1:], outs[1:]):
        send(new, out)
    for copy in copies:
        copy.wait()


def swap(values, axis, counts):
    sizes = [counts[name] for name in ("row", "col")]
    along = ("row", "col").index(axis)
    out = []
    for k, value in enumerate(values):
        moves = []
        for i in range(sizes[0] * sizes[1]):
            place = list(divmod(i, sizes[1]))
            target = list(place)
            here = place[along]
            if here % len(values) == k and here + 1 < sizes[along]:
                target[along] += 1
            elif (here - 1) % len(values) == k and here > 0:
                target[along] -= 1
            elif (place[1 - along] ^ 1) < sizes[1 - along]:
                target[1 - along] ^= 1
            else:
                continue
            moves.append((i, target[0] * sizes[1] + target[1]))
        out.append(lax.ppermute(value, ("row", "col"), moves))
    return out


def solution(mesh):
    counts = (mesh.shape["row"], mesh.shape["col"])

    def local(relief):
        shape = bands, n, m = relief.shape
        levels = [jax.ShapeDtypeStruct((bands, n >> k, m >> k), F32) for k in range(1, LEVELS + 1)]
        width = 128 * slots(bands, m)[1]
        row_part = jax.ShapeDtypeStruct((8, width), F32)
        col_part = jax.ShapeDtypeStruct((16, 128), F32)
        rim = jax.ShapeDtypeStruct((bands, 128, 128), F32)
        tall = [
            jax.ShapeDtypeStruct((bands, (lanes_of(m >> k) if k else m) // 128, PAD + (n >> k) + TAIL, 128), F32)
            for k in range(LEVELS)
        ]
        send_e, send_o, field, *mats = pl.pallas_call(
            functools.partial(edge_kernel, shape, counts),
            out_shape=[
                row_part, row_part, tall[0],
                jax.ShapeDtypeStruct((4, 256, 256), BF16),
                jax.ShapeDtypeStruct((128, 256), BF16),
                jax.ShapeDtypeStruct((m >> 2, m >> 3), BF16),
            ],
            in_specs=[pl.BlockSpec(memory_space=pltpu.HBM)],
            out_specs=[VMEM] * 6,
            scratch_shapes=[
                pltpu.VMEM((lanes_of(m >> k) // 128, bands * 40, 128), F32) for k in range(1, LEVELS)
            ] + [
                pltpu.VMEM((8, width), F32),
                pltpu.VMEM((8, width), F32),
                pltpu.SemaphoreType.DMA((2,)),
            ],
            compiler_params=pltpu.CompilerParams(vmem_limit_bytes=LIMIT),
            name="edge",
        )(pltpu.with_memory_space_constraint(relief, pltpu.HBM))
        *own, rim_a, rim_b = pl.pallas_call(
            functools.partial(pyramid_kernel, shape, counts),
            out_shape=tall[1:] + [levels[-1], rim, rim],
            in_specs=[VMEM] * 4,
            out_specs=[VMEM] * 6,
            compiler_params=pltpu.CompilerParams(vmem_limit_bytes=LIMIT),
            cost_estimate=pl.CostEstimate(flops=8_000_000_000, bytes_accessed=0, transcendentals=0),
            name="pyramid",
        )(field, *mats)
        row_e, row_o = swap((send_e, send_o), "row", mesh.shape)
        sends = pl.pallas_call(
            functools.partial(rim_kernel, shape, counts),
            out_shape=[col_part] * 3,
            in_specs=[VMEM] * 4,
            out_specs=[VMEM] * 3,
            scratch_shapes=[pltpu.VMEM((bands, 128, 128), F32)] * 2,
            compiler_params=pltpu.CompilerParams(vmem_limit_bytes=4 << 20),
            name="rim",
        )(rim_a, rim_b, row_e, row_o)
        cols = swap(sends, "col", mesh.shape)
        ends = jax.ShapeDtypeStruct((bands, n >> 1, 256), F32)
        hbm = pl.BlockSpec(memory_space=pltpu.HBM)
        out, *done = pl.pallas_call(
            functools.partial(settle_kernel, shape),
            out_shape=[levels[0], ends] + levels[1:],
            in_specs=[VMEM] * 6,
            out_specs=[hbm] + [VMEM] * 4,
            scratch_shapes=[
                pltpu.VMEM((bands, n >> 1, (m >> 1) - 256), F32), pltpu.SemaphoreType.DMA((bands,)),
            ],
            compiler_params=pltpu.CompilerParams(vmem_limit_bytes=8 << 20),
            cost_estimate=pl.CostEstimate(flops=2_000_000_000, bytes_accessed=0, transcendentals=0),
            name="settle",
        )(*own, row_e, row_o)
        return tuple(pl.pallas_call(
            functools.partial(finish_kernel, shape),
            out_shape=levels,
            in_specs=[hbm] + [VMEM] * 7,
            out_specs=[hbm] * 4,
            scratch_shapes=[pltpu.VMEM((bands, 128, 128), F32)] * 2 + [
                pltpu.VMEM(level.shape, F32) for level in [ends] + levels[1:]
            ] + [pltpu.SemaphoreType.DMA((2 * bands + LEVELS - 1,))],
            input_output_aliases={0: 0},
            compiler_params=pltpu.CompilerParams(vmem_limit_bytes=8 << 20),
            name="finish",
        )(out, *done, *cols))

    placed = P(None, "row", "col")
    return jax.shard_map(
        local, mesh=mesh, in_specs=(placed,), out_specs=(placed,) * LEVELS, check_vma=False
    )
```
